512 devices in a mesh: grp: 8 (over z), limb: 64 (over x, y, core).
Axes of the slice: x: 4, y: 8, z: 8, core: 2. Of those that a mesh axis runs over, the one named last changes fastest.
Arguments:
- digits: float32 [32, 3, 16, 65536], P('grp', None, None, 'limb'), may hold values from 0 to 2047, as said below
- keys: float32 [32, 3, 2, 16, 65536], P('grp', None, None, None, 'limb'), may hold values from 0 to 2047, as said below
- requests: int32 [32, 32], P('grp'), may hold values from 0 to 1, as said below
- rotations: int32 [32], replicated, may hold values from 1 to 256, as said below
- moduli: int32 [16], replicated, may hold values from 2048 to 4095
Outputs:
- switched: float32 [32, 2, 16, 65536], P('grp', None, None, 'limb')
The draws below stay inside these ranges and needn't reach their ends.
Inputs may be any that keep to these rules, and one draw needn't show every extreme that they name: `digits`: every entry is an integer. `keys`: every entry is an integer. `requests`: for each block of ciphertexts k * 4 to (k + 1) * 4 - 1 and each owner group's keys g * 4 to (g + 1) * 4 - 1, between 1 and 2 of those ciphertexts request one or more of those keys; in every draw some owner group is requested by exactly 2 ciphertexts of every block. `rotations`: the largest amount is exactly 256.
All inputs are finite; a program needn't handle non-finite values.
Results may differ from the reference program's by a relative error of at most 0.0003.
Values sent between devices are 32-bit elements; how exact they have to be, the bound alone decides.
A program may use at most 64 MiB of HBM per device.

```python
import jax
import jax.numpy as jnp
from jax import lax

NCOEF = 65536
DNUM = 3
LIMBS = 16
KEYS_GRP = 4
RMAX = 256
CT_GRP = 4
CAP = 2
CTS = 32
KEYS = 32


def draw_digits(key, part):
    return jax.random.randint(key, (CTS, DNUM, LIMBS, NCOEF), 0, 2048).astype(jnp.float32)


def draw_keys(key, part):
    return jax.random.randint(key, (KEYS, DNUM, 2, LIMBS, NCOEF), 0, 2048).astype(jnp.float32)


def draw_requests(key, part):
    groups = CTS // CT_GRP
    count_key, busy_key, score_key, subset_key = jax.random.split(key, 4)
    counts = jax.random.randint(count_key, (groups, groups), 1, CAP + 1)
    busiest = jax.random.randint(busy_key, (), 0, groups)
    counts = jnp.where(jnp.arange(groups)[None, :] == busiest, CAP, counts)
    scores = jax.random.randint(score_key, (groups, groups, CT_GRP), 0, 1048576) * CT_GRP + jnp.arange(CT_GRP)
    ranking = jnp.argsort(jnp.argsort(scores, axis=2, stable=True), axis=2, stable=True)
    chosen = (ranking < counts[:, :, None]).astype(jnp.int32)
    subsets = jax.random.randint(subset_key, (groups, groups, CT_GRP), 1, 2 ** KEYS_GRP)
    powers = 2 ** jnp.arange(KEYS_GRP)
    key_bits = subsets[..., None] // powers % 2
    request = chosen[..., None] * key_bits
    return jnp.transpose(request, (0, 2, 1, 3)).reshape(CTS, KEYS).astype(jnp.int32)


def draw_rotations(key, part):
    amount_key, place_key = jax.random.split(key)
    amounts = jax.random.randint(amount_key, (KEYS,), 1, RMAX + 1)
    largest_at = jax.random.randint(place_key, (), 0, KEYS)
    return jnp.where(jnp.arange(KEYS) == largest_at, RMAX, amounts).astype(jnp.int32)


def draw_moduli(key, part):
    return jax.random.randint(key, (LIMBS,), 2048, 4096).astype(jnp.int32)


def setup_inputs(seed: int = 0) -> dict:
    splits = jax.random.split(jax.random.key(seed), 6)
    digits = draw_digits(jax.random.fold_in(splits[5], 71), 0)
    keys = draw_keys(jax.random.fold_in(splits[5], 71), 0)
    requests = draw_requests(jax.random.fold_in(splits[5], 71), 0)
    rotations = draw_rotations(jax.random.fold_in(splits[5], 71), 0)
    moduli = draw_moduli(jax.random.fold_in(splits[5], 71), 0)
    return {"digits": digits, "keys": keys, "requests": requests, "rotations": rotations, "moduli": moduli}


def reduce_mod(amount, modulus):
    quotient = jnp.floor(amount * (1.0 / modulus))
    remainder = amount - quotient * modulus
    remainder = jnp.where(remainder < 0, remainder + modulus, remainder)
    return jnp.where(remainder >= modulus, remainder - modulus, remainder)


def reference(digits, keys, requests, rotations, moduli):
    modulus = moduli.astype(jnp.float32)[:, None]

    def one_cipher(operands):
        cipher_digits, wanted = operands

        def add_key(running, scanned):
            key_block, amount, wanted_flag = scanned
            combined = jnp.sum(cipher_digits[:, None] * key_block, axis=0)
            product = reduce_mod(combined, modulus)
            rotated = jnp.roll(product, -2 * amount, axis=-1)
            return running + wanted_flag.astype(jnp.float32) * rotated, None

        initial = jnp.zeros((2, LIMBS, NCOEF), jnp.float32)
        running, unused = lax.scan(add_key, initial, (keys, rotations, wanted))
        return reduce_mod(running, modulus) / modulus

    return lax.map(one_cipher, (digits, requests))
```

```python
import jax
import jax.numpy as jnp
from jax import lax
from jax.experimental import pallas as pl
from jax.experimental.pallas import tpu as pltpu
from jax.sharding import PartitionSpec as P

MESH = pl.DeviceIdType.MESH
LINE = 4
HALF = 8
WIDE = 512


def reduce_mod(amount, modulus):
    quotient = jnp.floor(amount * (1.0 / modulus))
    remainder = amount - quotient * modulus
    remainder = jnp.where(remainder < 0, remainder + modulus, remainder)
    return jnp.where(remainder >= modulus, remainder - modulus, remainder)


def kernel(groups, limbs, rot, digits, keys, consts, out,
           dall, kall, fall, main, rim_out, part_in, rim_in,
           d_send, d_recv, f_send, f_recv, k_send, k_recv, r_send, r_recv,
           o_send, o_recv, d_local, k_local):
    z = lax.axis_index("grp")
    lb = lax.axis_index("limb")
    before = lax.rem(lb + limbs - 1, limbs)
    after = lax.rem(lb + 1, limbs)
    columns = digits.shape[-1]
    cts = digits.shape[0]
    nkeys = keys.shape[0]

    def zmod(value):
        return lax.rem(value, groups)

    def pos(a):
        return lax.rem(z + 2 * a, LINE)

    q0 = pos(0)
    ae = lax.rem((q0 + 1) // 2, 2)
    am = 1 - ae
    qe = pos(ae)
    he = qe // 2
    z_out = zmod(z + groups - 1 + 2 * he)
    z_far = zmod(z + groups - 2 + 4 * he)

    def own_digits(a, ct):
        return digits.at[ct, :, pl.ds(pl.multiple_of(HALF * a, HALF), HALF), :]

    def own_keys(a, key):
        return keys.at[key, :, :, pl.ds(pl.multiple_of(HALF * a, HALF), HALF), :]

    def remote(src, dst, send, recv, zt, lt):
        return pltpu.make_async_remote_copy(
            src_ref=src, dst_ref=dst, send_sem=send, recv_sem=recv,
            device_id=(zt, lt), device_id_type=MESH)

    def d_copy(a, d, ct, way, own=False):
        src = own_digits(a, ct) if own else dall.at[a, d, ct]
        return remote(src, dall.at[a, d, ct], d_send.at[a, way, d, ct], d_recv.at[a, d, ct],
                      zmod(z + 1 + (groups - 2) * way), lb)

    def f_copy(a, d, way):
        return remote(fall.at[a, d], fall.at[a, d], f_send.at[a, way, d], f_recv.at[a, d],
                      zmod(z + 1 + (groups - 2) * way), lb)

    def k_copy(a, key):
        q = pos(a)
        slot = 1 + 2 * lax.rem((q + 1) // 2, 2)
        return remote(own_keys(a, key), kall.at[a, slot, key], k_send.at[a, key],
                      k_recv.at[a, slot, key], zmod(z + groups - 1 + 2 * (q // 2)), lb)

    def k_forward(key):
        return remote(kall.at[ae, 3, key], kall.at[ae, 2, key], k_send.at[2, key],
                      k_recv.at[ae, 2, key], z_out, lb)

    def k_arrive(slot, key):
        remote(kall.at[ae, slot, key], kall.at[ae, slot, key], k_send.at[2, key],
               k_recv.at[ae, slot, key], z_out, lb).wait_recv()

    def r_copy(a, d, ct):
        return remote(rim_out.at[a, d, ct], rim_in.at[a, d, ct], r_send.at[a, d, ct],
                      r_recv.at[a, d, ct], z, before)

    def o_copy(a, way, d, ct):
        return remote(main.at[a, d, ct], part_in.at[a, way, d, ct], o_send.at[a, d, ct],
                      o_recv.at[a, way, d, ct], zmod(z + 1 + (groups - 2) * way), lb)

    def local_d(a, ct):
        return pltpu.make_async_copy(own_digits(a, ct), dall.at[a, pos(a), ct], d_local.at[a, ct])

    def local_k(a, key):
        return pltpu.make_async_copy(own_keys(a, key), kall.at[a, 0, key], k_local.at[a, key])

    def loop(count, body):
        lax.fori_loop(0, count, lambda i, c: (body(i), c)[1], 0)

    def compute(a, d, ct, slot, zg):
        flags = pltpu.roll(fall[a, d], lax.rem(256 - 32 * ct - nkeys * zg, 128), 1)
        m = jnp.concatenate([consts[1 + a]] * (columns // 128), axis=1)
        inv = jnp.concatenate([consts[3 + a]] * (columns // 128), axis=1)
        pad = jnp.zeros((HALF, WIDE), jnp.float32)
        for p in range(2):
            total = jnp.zeros((HALF, WIDE + columns), jnp.float32)
            for key in range(nkeys):
                x = dall[a, d, ct, 0] * kall[a, slot, key, 0, p]
                x = x + dall[a, d, ct, 1] * kall[a, slot, key, 1, p]
                x = x + dall[a, d, ct, 2] * kall[a, slot, key, 2, p]
                t = (x - jnp.floor(x * inv) * m) * flags[:, key:key + 1]
                shift = WIDE + columns - 2 * rot[nkeys * zg + key]
                total = total + pltpu.roll(jnp.concatenate([pad, t], axis=1), shift, 1)
            rim_out[a, d, ct, p] = rim_out[a, d, ct, p] + total[:, :WIDE]
            main[a, d, ct, p] = main[a, d, ct, p] + total[:, WIDE:]

    def start_local(i):
        local_d(i // cts, lax.rem(i, cts)).start()
        local_k(i // cts, lax.rem(i, cts)).start()
    loop(2 * cts, start_local)
    for a in range(2):
        fall[a, pos(a)] = consts[0]
    barrier = pltpu.get_barrier_semaphore()
    for zt, lt in ((zmod(z + 1), lb), (zmod(z + groups - 1), lb), (z, before), (z, after)):
        pl.semaphore_signal(barrier, inc=1, device_id=(zt, lt), device_id_type=MESH)
    pl.semaphore_wait(barrier, 4)

    for a in range(2):
        @pl.when(pos(a) < LINE - 1)
        def _():
            f_copy(a, pos(a), 0).start()

        @pl.when(pos(a) > 0)
        def _():
            f_copy(a, pos(a), 1).start()

    def send_own(i):
        a, ct = i // cts, lax.rem(i, cts)

        @pl.when(pos(a) < LINE - 1)
        def _():
            d_copy(a, pos(a), ct, 0, True).start()

        @pl.when(pos(a) > 0)
        def _():
            d_copy(a, pos(a), ct, 1, True).start()
    loop(2 * cts, send_own)
    loop(2 * nkeys, lambda i: k_copy(i // nkeys, lax.rem(i, nkeys)).start())

    def clear(i):
        a, d, ct = i // (LINE * cts), lax.rem(i // cts, LINE), lax.rem(i, cts)
        main[a, d, ct] = jnp.zeros(main.shape[3:], jnp.float32)
        rim_out[a, d, ct] = jnp.zeros(rim_out.shape[3:], jnp.float32)
    loop(2 * LINE * cts, clear)

    def wait_local(i):
        local_d(i // cts, lax.rem(i, cts)).wait()
        local_k(i // cts, lax.rem(i, cts)).wait()
    loop(2 * cts, wait_local)

    def own_block(i):
        a, ct = i // cts, lax.rem(i, cts)
        compute(a, pos(a), ct, 0, z)

        @pl.when(a == am)
        def _():
            r_copy(a, pos(a), ct).start()
    loop(2 * cts, own_block)

    def gathered(s, i, slots):
        way, ct, a = lax.rem(i, 2), lax.rem(i // 2, cts), i // (2 * cts)
        q = pos(a)
        d = q + (2 * way - 1) * s

        @pl.when((d >= 0) & (d < LINE))
        def _():
            d_copy(a, d, ct, way).wait_recv()
            onward = (1 - way) * (LINE - 1 - q) + way * q > 0

            @pl.when(onward)
            def _():
                d_copy(a, d, ct, way).start()

            @pl.when(ct == 0)
            def _():
                f_copy(a, d, way).wait_recv()

                @pl.when(onward)
                def _():
                    f_copy(a, d, way).start()

            if slots == 1:
                compute(a, d, ct, 0, z)
            else:
                ends = 1 - (a - ae) * (a - ae)

                def one(slot):
                    compute(a, d, ct, slot, z * (1 - slot) + z_out * slot)
                loop(1 + ends, one)

            @pl.when(a == am)
            def _():
                r_copy(a, d, ct).start()

    per_step = 4 * cts
    loop(per_step, lambda i: gathered(1, i, 1))

    def relay(key):
        k_arrive(3, key)
        k_forward(key).start()
    loop(nkeys, relay)
    loop(nkeys, lambda key: k_arrive(1, key))

    def near_keys(i):
        step, ct = i // cts, lax.rem(i, cts)
        compute(ae, qe + step * (1 - 2 * he), ct, 1, z_out)
    loop(2 * cts, near_keys)

    loop(2 * per_step, lambda i: gathered(2 + i // per_step, lax.rem(i, per_step), 2))
    loop(nkeys, lambda key: k_arrive(2, key))

    def add_rim(a, d, ct):
        r_copy(a, d, ct).wait_recv()
        main[a, d, ct, :, :, columns - WIDE:] = (
            main[a, d, ct, :, :, columns - WIDE:] + rim_in[a, d, ct])

    def add_part(a, way, d, ct):
        o_copy(a, way, d, ct).wait_recv()
        main[a, d, ct] = main[a, d, ct] + part_in[a, way, d, ct]

    def last_keys(step, ct):
        d = (LINE - 1 - step) * (1 - he) + step * he
        compute(ae, d, ct, 2, z_far)
        r_copy(ae, d, ct).start()

    def pass_on(step, i):
        way, ct, a = lax.rem(i, 2), lax.rem(i // 2, cts), i // (2 * cts)
        q = pos(a)
        d = (LINE - 1 - step) * (1 - way) + step * way

        @pl.when((d - q) * (1 - 2 * way) > 0)
        def _():
            add_rim(a, d, ct)

            @pl.when((1 - way) * q + way * (LINE - 1 - q) > 0)
            def _():
                add_part(a, way, d, ct)
            o_copy(a, way, d, ct).start()

    def tail(step):
        @pl.when(step < LINE)
        def _():
            loop(cts, lambda ct: last_keys(step, ct))

        @pl.when(step > 0)
        def _():
            loop(4 * cts, lambda i: pass_on(step - 1, i))
    loop(LINE, tail)

    def finish(i):
        a, ct = i // cts, lax.rem(i, cts)
        q = pos(a)
        add_rim(a, q, ct)

        @pl.when(q > 0)
        def _():
            add_part(a, 0, q, ct)

        @pl.when(q < LINE - 1)
        def _():
            add_part(a, 1, q, ct)
        out[ct, :, pl.ds(pl.multiple_of(HALF * a, HALF), HALF), :] = main[a, q, ct]
    loop(2 * cts, finish)

    def drain(i):
        a, d, ct = i // (LINE * cts), lax.rem(i // cts, LINE), lax.rem(i, cts)
        q = pos(a)
        r_copy(a, d, ct).wait_send()

        @pl.when((q < LINE - 1) & (d <= q))
        def _():
            d_copy(a, d, ct, 0).wait_send()

            @pl.when(ct == 0)
            def _():
                f_copy(a, d, 0).wait_send()

        @pl.when((q > 0) & (d >= q))
        def _():
            d_copy(a, d, ct, 1).wait_send()

            @pl.when(ct == 0)
            def _():
                f_copy(a, d, 1).wait_send()

        @pl.when((d < q) | (d > q))
        def _():
            o_copy(a, 0, d, ct).wait_send()
    loop(2 * LINE * cts, drain)
    loop(2 * nkeys, lambda i: k_copy(i // nkeys, lax.rem(i, nkeys)).wait_send())
    loop(nkeys, lambda key: k_forward(key).wait_send())


def per_device(digits, keys, requests, rotations, moduli):
    groups, limbs = lax.axis_size("grp"), lax.axis_size("limb")
    cts, dnum, limb_count, columns = digits.shape
    nkeys = keys.shape[0]
    modulus = moduli.astype(jnp.float32)
    flags = jnp.broadcast_to(requests.astype(jnp.float32).reshape(1, 1, 128), (1, HALF, 128))
    mods = jnp.broadcast_to(modulus.reshape(2, HALF, 1), (2, HALF, 128))
    consts = jnp.concatenate([flags, mods, 1.0 / mods], axis=0)
    f32 = jnp.float32
    dma = pltpu.SemaphoreType.DMA
    any_space = pl.BlockSpec(memory_space=pl.ANY)
    total = pl.pallas_call(
        lambda *refs: kernel(groups, limbs, *refs),
        out_shape=jax.ShapeDtypeStruct((cts, 2, limb_count, columns), f32),
        in_specs=[pl.BlockSpec(memory_space=pltpu.SMEM), any_space, any_space,
                  pl.BlockSpec(memory_space=pltpu.VMEM)],
        out_specs=pl.BlockSpec(memory_space=pltpu.VMEM),
        scratch_shapes=[
            pltpu.VMEM((2, LINE, cts, dnum, HALF, columns), f32),
            pltpu.VMEM((2, 4, nkeys, dnum, 2, HALF, columns), f32),
            pltpu.VMEM((2, LINE, HALF, 128), f32),
            pltpu.VMEM((2, LINE, cts, 2, HALF, columns), f32),
            pltpu.VMEM((2, LINE, cts, 2, HALF, WIDE), f32),
            pltpu.VMEM((2, 2, LINE, cts, 2, HALF, columns), f32),
            pltpu.VMEM((2, LINE, cts, 2, HALF, WIDE), f32),
            dma((2, 2, LINE, cts)), dma((2, LINE, cts)),
            dma((2, 2, LINE)), dma((2, LINE)),
            dma((3, nkeys)), dma((2, 4, nkeys)),
            dma((2, LINE, cts)), dma((2, LINE, cts)),
            dma((2, LINE, cts)), dma((2, 2, LINE, cts)),
            dma((2, cts)), dma((2, nkeys)),
        ],
        compiler_params=pltpu.CompilerParams(
            collective_id=0, has_side_effects=True, vmem_limit_bytes=60 * 1024 * 1024),
        name="keyswitch",
    )(rotations, digits, keys, consts)
    column = modulus[:, None]
    return reduce_mod(total, column) / column


def solution(mesh):
    in_specs = (
        P("grp", None, None, "limb"),
        P("grp", None, None, None, "limb"),
        P("grp", None),
        P(),
        P(),
    )
    out_specs = P("grp", None, None, "limb")
    return jax.shard_map(
        per_device, mesh=mesh, in_specs=in_specs, out_specs=out_specs, check_vma=False
    )
```

```python
import jax
import jax.numpy as jnp
from jax import lax
from jax.experimental import pallas as pl
from jax.experimental.pallas import tpu as pltpu
from jax.sharding import PartitionSpec as P

MESH = pl.DeviceIdType.MESH
LINE = 4
HALF = 8
WIDE = 512
GROUP = 2


def reduce_mod(amount, modulus):
    quotient = jnp.floor(amount * (1.0 / modulus))
    remainder = amount - quotient * modulus
    remainder = jnp.where(remainder < 0, remainder + modulus, remainder)
    return jnp.where(remainder >= modulus, remainder - modulus, remainder)


def kernel(groups, limbs, rot, mods, digits, keys, requests, out,
           consts, flag, dall, kall, fall, main, rim_out, part_in, rim_in,
           d_send, d_recv, f_send, f_recv, k_send, k_recv, r_send, r_recv,
           o_send, o_recv, d_local, k_local):
    z = lax.axis_index("grp")
    lb = lax.axis_index("limb")
    before = lax.rem(lb + limbs - 1, limbs)
    after = lax.rem(lb + 1, limbs)
    columns = digits.shape[-1]
    cts = digits.shape[0]
    nkeys = keys.shape[0]

    def zmod(value):
        return lax.rem(value, groups)

    def pos(a):
        return lax.rem(z + 2 * a, LINE)

    q0 = pos(0)
    ae = lax.rem((q0 + 1) // 2, 2)
    am = 1 - ae
    qe = pos(ae)
    he = qe // 2
    z_out = zmod(z + groups - 1 + 2 * he)
    z_far = zmod(z + groups - 2 + 4 * he)

    parts = cts // GROUP

    def several(h):
        return pl.ds(GROUP * h, GROUP)

    def own_digits(a, h):
        return digits.at[several(h), :, pl.ds(pl.multiple_of(HALF * a, HALF), HALF), :]

    def own_keys(a, key):
        return keys.at[key, :, :, pl.ds(pl.multiple_of(HALF * a, HALF), HALF), :]

    def remote(src, dst, send, recv, zt, lt):
        return pltpu.make_async_remote_copy(
            src_ref=src, dst_ref=dst, send_sem=send, recv_sem=recv,
            device_id=(zt, lt), device_id_type=MESH)

    def d_copy(a, d, h, way, own=False):
        here = dall.at[a, d, several(h)]
        return remote(own_digits(a, h) if own else here, here, d_send.at[a, way, d, h],
                      d_recv.at[a, d, h], zmod(z + 1 + (groups - 2) * way), lb)

    def f_copy(a, d, way):
        return remote(fall.at[a, d], fall.at[a, d], f_send.at[a, way, d], f_recv.at[a, d],
                      zmod(z + 1 + (groups - 2) * way), lb)

    def k_copy(a, key):
        q = pos(a)
        slot = 1 + 2 * lax.rem((q + 1) // 2, 2)
        return remote(own_keys(a, key), kall.at[a, slot, key], k_send.at[a, key],
                      k_recv.at[a, slot, key], zmod(z + groups - 1 + 2 * (q // 2)), lb)

    def k_forward(key):
        return remote(kall.at[ae, 3, key], kall.at[ae, 2, key], k_send.at[2, key],
                      k_recv.at[ae, 2, key], z_out, lb)

    def k_arrive(slot, key):
        remote(kall.at[ae, slot, key], kall.at[ae, slot, key], k_send.at[2, key],
               k_recv.at[ae, slot, key], z_out, lb).wait_recv()

    def r_copy(a, d, h):
        return remote(rim_out.at[a, d, several(h)], rim_in.at[a, d, several(h)],
                      r_send.at[a, d, h], r_recv.at[a, d, h], z, before)

    def o_copy(a, way, d, h):
        return remote(main.at[a, d, several(h)], part_in.at[a, way, d, several(h)],
                      o_send.at[a, d, h], o_recv.at[a, way, d, h],
                      zmod(z + 1 + (groups - 2) * way), lb)

    def local_d(a, h):
        return pltpu.make_async_copy(own_digits(a, h), dall.at[a, pos(a), several(h)],
                                     d_local.at[a, h])

    def local_k(a, key):
        return pltpu.make_async_copy(own_keys(a, key), kall.at[a, 0, key], k_local.at[a, key])

    def loop(count, body):
        lax.fori_loop(0, count, lambda i, c: (body(i), c)[1], 0)

    def compute(a, d, ct, slot, zg):
        flags = pltpu.roll(fall[a, d], lax.rem(256 - 32 * ct - nkeys * zg, 128), 1)
        m = jnp.concatenate([consts[a]] * (columns // 128), axis=1)
        inv = jnp.concatenate([consts[2 + a]] * (columns // 128), axis=1)
        pad = jnp.zeros((HALF, WIDE), jnp.float32)
        for p in range(2):
            total = jnp.zeros((HALF, WIDE + columns), jnp.float32)
            for key in range(nkeys):
                x = dall[a, d, ct, 0] * kall[a, slot, key, 0, p]
                x = x + dall[a, d, ct, 1] * kall[a, slot, key, 1, p]
                x = x + dall[a, d, ct, 2] * kall[a, slot, key, 2, p]
                t = (x - jnp.floor(x * inv) * m) * flags[:, key:key + 1]
                shift = WIDE + columns - 2 * rot[nkeys * zg + key]
                total = total + pltpu.roll(jnp.concatenate([pad, t], axis=1), shift, 1)
            rim_out[a, d, ct, p] = rim_out[a, d, ct, p] + total[:, :WIDE]
            main[a, d, ct, p] = main[a, d, ct, p] + total[:, WIDE:]

    def compute_group(a, d, h, slot, zg):
        loop(GROUP, lambda c: compute(a, d, GROUP * h + c, slot, zg))

    loop(2 * parts, lambda i: local_d(i // parts, lax.rem(i, parts)).start())
    loop(2 * nkeys, lambda i: local_k(i // nkeys, lax.rem(i, nkeys)).start())
    barrier = pltpu.get_barrier_semaphore()
    for zt, lt in ((zmod(z + 1), lb), (zmod(z + groups - 1), lb), (z, before), (z, after)):
        pl.semaphore_signal(barrier, inc=1, device_id=(zt, lt), device_id_type=MESH)

    row = lax.broadcasted_iota(jnp.int32, (HALF, 128), 0)
    for a in range(2):
        m = jnp.ones((HALF, 128), jnp.float32)
        for limb in range(HALF):
            m = jnp.where(row == limb, mods[HALF * a + limb].astype(jnp.float32), m)
        consts[a] = m
        consts[2 + a] = 1.0 / m
    flag[...] = jnp.zeros_like(flag)
    flag[:cts, :requests.shape[1]] = requests[...].astype(jnp.float32)
    wanted = jnp.zeros((HALF, 128), jnp.float32)
    for ct in range(cts):
        spread = jnp.broadcast_to(flag[ct:ct + 1, :], (HALF, 128))
        wanted = wanted + pltpu.roll(spread, 32 * ct, 1)
    for a in range(2):
        fall[a, pos(a)] = wanted
    pl.semaphore_wait(barrier, 4)

    def send_own(i):
        a, h = i // parts, lax.rem(i, parts)

        @pl.when(pos(a) < LINE - 1)
        def _():
            d_copy(a, pos(a), h, 0, True).start()

        @pl.when(pos(a) > 0)
        def _():
            d_copy(a, pos(a), h, 1, True).start()
    loop(2 * parts, send_own)
    for a in range(2):
        @pl.when(pos(a) < LINE - 1)
        def _():
            f_copy(a, pos(a), 0).start()

        @pl.when(pos(a) > 0)
        def _():
            f_copy(a, pos(a), 1).start()
    loop(2 * nkeys, lambda i: k_copy(i // nkeys, lax.rem(i, nkeys)).start())

    def clear(i):
        a, d, ct = i // (LINE * cts), lax.rem(i // cts, LINE), lax.rem(i, cts)
        main[a, d, ct] = jnp.zeros(main.shape[3:], jnp.float32)
        rim_out[a, d, ct] = jnp.zeros(rim_out.shape[3:], jnp.float32)
    loop(2 * LINE * cts, clear)
    loop(2 * parts, lambda i: local_d(i // parts, lax.rem(i, parts)).wait())
    loop(2 * nkeys, lambda i: local_k(i // nkeys, lax.rem(i, nkeys)).wait())

    def own_block(i):
        a, h = i // parts, lax.rem(i, parts)
        compute_group(a, pos(a), h, 0, z)

        @pl.when(a == am)
        def _():
            r_copy(a, pos(a), h).start()
    loop(2 * parts, own_block)

    def gathered(s, i, slots):
        way, h, a = lax.rem(i, 2), lax.rem(i // 2, parts), i // (2 * parts)
        q = pos(a)
        d = q + (2 * way - 1) * s

        @pl.when((d >= 0) & (d < LINE))
        def _():
            d_copy(a, d, h, way).wait_recv()
            onward = (1 - way) * (LINE - 1 - q) + way * q > 0

            @pl.when(onward)
            def _():
                d_copy(a, d, h, way).start()

            @pl.when(h == 0)
            def _():
                f_copy(a, d, way).wait_recv()

                @pl.when(onward)
                def _():
                    f_copy(a, d, way).start()

            if slots == 1:
                compute_group(a, d, h, 0, z)
            else:
                ends = 1 - (a - ae) * (a - ae)

                def one(slot):
                    compute_group(a, d, h, slot, z * (1 - slot) + z_out * slot)
                loop(1 + ends, one)

            @pl.when(a == am)
            def _():
                r_copy(a, d, h).start()

    per_step = 4 * parts
    loop(per_step, lambda i: gathered(1, i, 1))

    def relay(key):
        k_arrive(3, key)
        k_forward(key).start()
    loop(nkeys, relay)
    loop(nkeys, lambda key: k_arrive(1, key))

    def near_keys(i):
        step, h = i // parts, lax.rem(i, parts)
        compute_group(ae, qe + step * (1 - 2 * he), h, 1, z_out)
    loop(2 * parts, near_keys)

    loop(2 * per_step, lambda i: gathered(2 + i // per_step, lax.rem(i, per_step), 2))
    loop(nkeys, lambda key: k_arrive(2, key))

    hm = pos(am) - 1

    def chain(way, item):
        return (LINE - 1 - item) * (1 - way) + item * way

    def add_rim(a, d, h):
        r_copy(a, d, h).wait_recv()
        at = several(h)
        main[a, d, at, :, :, columns - WIDE:] = (
            main[a, d, at, :, :, columns - WIDE:] + rim_in[a, d, at])

    def add_part(a, way, d, h):
        o_copy(a, way, d, h).wait_recv()
        main[a, d, several(h)] = main[a, d, several(h)] + part_in[a, way, d, several(h)]

    def pass_on(way, d, h):
        add_rim(am, d, h)
        add_part(am, way, d, h)
        o_copy(am, way, d, h).start()

    def tail(i):
        step, h = i // parts, lax.rem(i, parts)
        compute_group(ae, chain(he, step), h, 2, z_far)
        r_copy(ae, chain(he, step), h).start()

        @pl.when(step > 0)
        def _():
            d = chain(he, step - 1)
            add_rim(ae, d, h)
            o_copy(ae, he, d, h).start()

        @pl.when(step > 1)
        def _():
            pass_on(hm, chain(hm, step - 2), h)

        @pl.when(step > 2)
        def _():
            pass_on(1 - hm, (LINE - 1) * hm, h)
    loop(LINE * parts, tail)

    def finish(a, h):
        q = pos(a)
        at = several(h)
        add_rim(a, q, h)

        @pl.when(q > 0)
        def _():
            add_part(a, 0, q, h)

        @pl.when(q < LINE - 1)
        def _():
            add_part(a, 1, q, h)
        out[at, :, pl.ds(pl.multiple_of(HALF * a, HALF), HALF), :] = main[a, q, at]
    loop(parts, lambda h: finish(am, h))
    loop(parts, lambda h: finish(ae, h))

    def drain(i):
        a, d, h = i // (LINE * parts), lax.rem(i // parts, LINE), lax.rem(i, parts)
        q = pos(a)
        r_copy(a, d, h).wait_send()

        @pl.when((q < LINE - 1) & (d <= q))
        def _():
            d_copy(a, d, h, 0).wait_send()

            @pl.when(h == 0)
            def _():
                f_copy(a, d, 0).wait_send()

        @pl.when((q > 0) & (d >= q))
        def _():
            d_copy(a, d, h, 1).wait_send()

            @pl.when(h == 0)
            def _():
                f_copy(a, d, 1).wait_send()

        @pl.when((d < q) | (d > q))
        def _():
            o_copy(a, 0, d, h).wait_send()
    loop(2 * LINE * parts, drain)
    loop(2 * nkeys, lambda i: k_copy(i // nkeys, lax.rem(i, nkeys)).wait_send())
    loop(nkeys, lambda key: k_forward(key).wait_send())


def per_device(digits, keys, requests, rotations, moduli):
    groups, limbs = lax.axis_size("grp"), lax.axis_size("limb")
    cts, dnum, limb_count, columns = digits.shape
    nkeys = keys.shape[0]
    modulus = moduli.astype(jnp.float32)
    parts = cts // GROUP
    f32 = jnp.float32
    dma = pltpu.SemaphoreType.DMA
    smem = pl.BlockSpec(memory_space=pltpu.SMEM)
    vmem = pl.BlockSpec(memory_space=pltpu.VMEM)
    any_space = pl.BlockSpec(memory_space=pl.ANY)
    total = pl.pallas_call(
        lambda *refs: kernel(groups, limbs, *refs),
        out_shape=jax.ShapeDtypeStruct((cts, 2, limb_count, columns), f32),
        in_specs=[smem, smem, any_space, any_space, vmem],
        out_specs=vmem,
        scratch_shapes=[
            pltpu.VMEM((4, HALF, 128), f32),
            pltpu.VMEM((HALF, 128), f32),
            pltpu.VMEM((2, LINE, cts, dnum, HALF, columns), f32),
            pltpu.VMEM((2, 4, nkeys, dnum, 2, HALF, columns), f32),
            pltpu.VMEM((2, LINE, HALF, 128), f32),
            pltpu.VMEM((2, LINE, cts, 2, HALF, columns), f32),
            pltpu.VMEM((2, LINE, cts, 2, HALF, WIDE), f32),
            pltpu.VMEM((2, 2, LINE, cts, 2, HALF, columns), f32),
            pltpu.VMEM((2, LINE, cts, 2, HALF, WIDE), f32),
            dma((2, 2, LINE, parts)), dma((2, LINE, parts)),
            dma((2, 2, LINE)), dma((2, LINE)),
            dma((3, nkeys)), dma((2, 4, nkeys)),
            dma((2, LINE, parts)), dma((2, LINE, parts)),
            dma((2, LINE, parts)), dma((2, 2, LINE, parts)),
            dma((2, parts)), dma((2, nkeys)),
        ],
        compiler_params=pltpu.CompilerParams(
            collective_id=0, has_side_effects=True, vmem_limit_bytes=60 * 1024 * 1024),
        name="keyswitch",
    )(rotations, moduli, digits, keys, requests)
    column = modulus[:, None]
    return reduce_mod(total, column) / column


def solution(mesh):
    in_specs = (
        P("grp", None, None, "limb"),
        P("grp", None, None, None, "limb"),
        P("grp", None),
        P(),
        P(),
    )
    out_specs = P("grp", None, None, "limb")
    return jax.shard_map(
        per_device, mesh=mesh, in_specs=in_specs, out_specs=out_specs, check_vma=False
    )
```

```python
import jax
import jax.numpy as jnp
from jax import lax
from jax.experimental import pallas as pl
from jax.experimental.pallas import tpu as pltpu
from jax.sharding import PartitionSpec as P

MESH = pl.DeviceIdType.MESH
WIDE = 512
DEPTHS = 4
LIMBS = 4


def reduce_mod(amount, modulus):
    quotient = jnp.floor(amount * (1.0 / modulus))
    remainder = amount - quotient * modulus
    remainder = jnp.where(remainder < 0, remainder + modulus, remainder)
    return jnp.where(remainder >= modulus, remainder - modulus, remainder)


def place(r, c):
    return r * (r + 1) // 2 + c


CROSS = place(DEPTHS, 0)
SLOTS = CROSS + DEPTHS
LAST = DEPTHS - 1


def kernel(groups, limbs, rot, mods, digits, keys, requests, out,
           stage_d, stage_k, consts, flag, dbuf, kbuf, main, part_in, rim_out, rim_in,
           d_send, d_recv, k_send, k_recv, o_send, o_recv, r_send, r_recv, local):
    z = lax.axis_index("grp")
    lb = lax.axis_index("limb")
    before = lax.rem(lb + limbs - 1, limbs)
    after = lax.rem(lb + 1, limbs)
    cts, dnum = digits.shape[:2]
    nkeys = keys.shape[0]
    pages = cts * dnum
    rows = 2 * LIMBS
    f32 = jnp.float32

    def zmod(value):
        return lax.rem(value, groups)

    def side(r):
        return lax.rem(z + r, 2)

    def inward(r):
        return zmod(z + 1 + (groups - 2) * side(r))

    def outward(r):
        return zmod(z + groups - 1 + 2 * side(r))

    def quarter(r):
        at = r * (1 - side(r)) + (groups - 1 - r) * side(r)
        return zmod(at + groups - z) // 2

    sub = lax.broadcasted_iota(jnp.int32, (rows, WIDE), 0)
    lane = lax.broadcasted_iota(jnp.int32, (rows, WIDE), 1)
    low = sub < LIMBS

    def swap(x):
        return pltpu.roll(x, LIMBS, 0)

    def remote(src, dst, send, recv, zt, lt):
        return pltpu.make_async_remote_copy(
            src_ref=src, dst_ref=dst, send_sem=send, recv_sem=recv,
            device_id=(zt, lt), device_id_type=MESH)

    def d_copy(r, c):
        s = place(r, c)
        t = place(r + 1, c) if r < LAST else CROSS + c
        return remote(dbuf.at[s], dbuf.at[t], d_send.at[s], d_recv.at[t], inward(r), lb)

    def d_arrive(t):
        remote(dbuf.at[t], dbuf.at[t], d_send.at[0], d_recv.at[t], z, lb).wait_recv()

    def k_copy(r, c, p):
        s, t = place(r, c), place(r + 1, c)
        return remote(kbuf.at[s, p], kbuf.at[t, p], k_send.at[s, p], k_recv.at[t, p],
                      inward(r), lb)

    def k_arrive(r, c, p):
        t = place(r, c)
        remote(kbuf.at[t, p], kbuf.at[t, p], k_send.at[0, p], k_recv.at[t, p], z, lb).wait_recv()

    def view(ref, s, p, h):
        return ref.at[s, p] if h is None else ref.at[s, p, pl.ds(2 * h, 2)]

    def o_cross(c, p, h=None):
        s, t, e = CROSS + c, place(LAST, c), 0 if h is None else h
        return remote(view(main, s, p, h), view(part_in, t, p, h),
                      o_send.at[s, p, e], o_recv.at[t, p, e], inward(LAST), lb)

    def o_copy(r, c, p, h=None):
        s, t, e = place(r, c), place(r - 1, c), 0 if h is None else h
        return remote(view(main, s, p, h), view(part_in, t, p, h),
                      o_send.at[s, p, e], o_recv.at[t, p, e], outward(r), lb)

    def r_copy(s, p, h=None):
        e = 0 if h is None else h
        src, dst = rim_out.at[s, p], rim_in.at[s, p]
        if h is not None:
            src, dst = src.at[pl.ds(h, 1)], dst.at[pl.ds(h, 1)]
        return remote(src, dst, r_send.at[s, p, e], r_recv.at[s, p, e], z, before)

    def loop(count, body):
        lax.fori_loop(0, count, lambda i, c: (body(i), c)[1], 0)

    def tiled(x):
        return jnp.concatenate([x] * (WIDE // 128), axis=1)

    def unit(s, r, k, p, h=None):
        held = r * (r + 1) // 2 + k
        zk = zmod(z + groups + (k - r) * (1 - 2 * side(r)))
        m = tiled(consts[r])
        inv = tiled(consts[DEPTHS + r])

        def pair(h):
            flags = pltpu.roll(dbuf[s, pages, :, :128],
                               lax.rem(256 - 64 * h - nkeys * zk, 128), 1)
            rim = rim_out[s, p, h]
            for e in range(2):
                ct = 2 * h + e
                total = jnp.zeros((rows, WIDE), f32)
                inside = jnp.zeros((rows, WIDE), f32)
                for key in range(nkeys):
                    x = dbuf[s, dnum * ct] * kbuf[held, p, key, 0]
                    for j in range(1, dnum):
                        x = x + dbuf[s, dnum * ct + j] * kbuf[held, p, key, j]
                    wanted = flags[:, 32 * e + key:32 * e + key + 1]
                    t = (x - jnp.floor(x * inv) * m) * wanted
                    kept = WIDE - 2 * rot[nkeys * zk + key]
                    t = pltpu.roll(t, kept, 1)
                    total = total + t
                    inside = inside + jnp.where(lane < kept, t, 0.0)
                wrapped = total - inside
                turned = swap(wrapped)
                main[s, p, ct] = main[s, p, ct] + (inside + jnp.where(low, turned, 0.0))
                if e == 0:
                    rim = rim + jnp.where(low, 0.0, turned)
                else:
                    rim = rim + jnp.where(low, wrapped, 0.0)
            rim_out[s, p, h] = rim
        if h is None:
            loop(cts // 2, pair)
        else:
            pair(h)

    def both(body):
        loop(2, body)

    def rims(s):
        both(lambda p: r_copy(s, p).start())

    def add_rim(s, p, h=None):
        r_copy(s, p, h).wait_recv()

        def pair(h):
            rim = rim_in[s, p, h]
            main[s, p, 2 * h] = main[s, p, 2 * h] + jnp.where(low, 0.0, rim)
            main[s, p, 2 * h + 1] = main[s, p, 2 * h + 1] + jnp.where(low, 0.0, swap(rim))
        if h is None:
            loop(cts // 2, pair)
        else:
            pair(h)

    def add_part(s, p, h=None):
        whole = view(part_in, s, p, h)
        e = 0 if h is None else h
        remote(whole, whole, o_send.at[0, p, e], o_recv.at[s, p, e], z, lb).wait_recv()
        at = (s, p) if h is None else (s, p, pl.ds(2 * h, 2))
        main[at] = main[at] + part_in[at]

    copy_d = pltpu.make_async_copy(digits, stage_d, local.at[0])
    copy_k = pltpu.make_async_copy(keys, stage_k, local.at[1])
    copy_d.start()
    copy_k.start()
    barrier = pltpu.get_barrier_semaphore()
    for zt, lt in ((zmod(z + 1), lb), (zmod(z + groups - 1), lb), (z, before), (z, after)):
        pl.semaphore_signal(barrier, inc=1, device_id=(zt, lt), device_id_type=MESH)

    row = lax.broadcasted_iota(jnp.int32, (rows, 128), 0)
    flag[...] = jnp.zeros_like(flag)
    flag[:cts, :requests.shape[1]] = requests[...].astype(f32)
    wanted = jnp.zeros((rows, 128), f32)
    for ct in range(cts):
        wanted = wanted + pltpu.roll(jnp.broadcast_to(flag[ct:ct + 1, :], (rows, 128)), 32 * ct, 1)
    wanted = jnp.concatenate([wanted] + [jnp.zeros((rows, 128), f32)] * (WIDE // 128 - 1), axis=1)
    for r in range(DEPTHS):
        dbuf[place(r, r), pages] = wanted
        m = jnp.ones((rows, 128), f32)
        for limb in range(LIMBS):
            value = mods[LIMBS * quarter(r) + limb].astype(f32)
            m = jnp.where((row == limb) | (row == limb + LIMBS), value, m)
        consts[r] = m
        consts[DEPTHS + r] = 1.0 / m

    def folded(x, r):
        first = lax.rem(quarter(r), 2) == 0
        a, b = x[:, :WIDE], x[:, WIDE:]
        return jnp.where(low, jnp.where(first, a, swap(a)), jnp.where(first, swap(b), b))

    def tile(r):
        return pl.ds(pl.multiple_of(rows * (quarter(r) // 2), rows), rows)

    copy_d.wait()
    for r in range(DEPTHS):
        def fold_d(i):
            dbuf[place(r, r), i] = folded(stage_d[i // dnum, lax.rem(i, dnum), tile(r), :], r)
        loop(pages, fold_d)
    pl.semaphore_wait(barrier, 4)
    for r in (0, 1, 2, 3):
        d_copy(r, r).start()
    copy_k.wait()

    def fold_keys(r, p):
        def fold_k(i):
            key, j = i // dnum, lax.rem(i, dnum)
            kbuf[place(r, r), p, key, j] = folded(stage_k[key, j, p, tile(r), :], r)
        loop(nkeys * dnum, fold_k)
    for r, p in ((0, 0), (1, 0), (0, 1), (2, 0)):
        fold_keys(r, p)
        k_copy(r, r, p).start()
    for r, p in ((3, 0), (1, 1), (2, 1), (3, 1)):
        fold_keys(r, p)

    def clear(i):
        s, p = i // 2, lax.rem(i, 2)
        main[s, p] = jnp.zeros(main.shape[2:], f32)
        rim_out[s, p] = jnp.zeros(rim_out.shape[2:], f32)
    loop(2 * SLOTS, clear)

    def own(i):
        r, p = i // 2, lax.rem(i, 2)
        unit(r * (r + 3) // 2, r, r, p)
    loop(2 * DEPTHS, own)
    rims(place(0, 0))

    for r in range(DEPTHS - 1):
        d_arrive(place(r + 1, r))
        d_copy(r + 1, r).start()

    def from_next(i):
        r, p = 1 + i // 2, lax.rem(i, 2)
        unit(r * (r + 1) // 2 + r - 1, r, r, p)
    loop(2 * LAST, from_next)
    for r in range(1, DEPTHS):
        rims(place(r, r - 1))
    d_arrive(CROSS + LAST)
    both(lambda p: unit(CROSS + LAST, LAST, LAST, p))

    k_arrive(1, 0, 0)
    k_copy(1, 0, 0).start()
    k_arrive(2, 1, 0)
    k_copy(2, 1, 0).start()
    k_arrive(3, 2, 0)
    loop(LAST, lambda i: unit((i + 1) * (i + 4) // 2, i + 1, i, 0))
    r_copy(place(1, 1), 0).start()
    unit(CROSS + 3, LAST, 2, 0)

    d_arrive(place(2, 0))
    d_copy(2, 0).start()
    both(lambda p: unit(place(2, 0), 2, 2, p))
    rims(place(2, 0))
    k_arrive(2, 0, 0)
    k_copy(2, 0, 0).start()
    for r in (2, 1):
        k_copy(r, r, 1).start()
    k_arrive(1, 0, 1)
    k_copy(1, 0, 1).start()
    unit(place(2, 2), 2, 0, 0)
    r_copy(place(2, 2), 0).start()

    def cross_block(c):
        loop(3, lambda i: unit(CROSS + c, LAST, LAST - i, 0))
        unit(CROSS + c, LAST, LAST, 1)

    d_arrive(place(3, 1))
    d_copy(3, 1).start()
    both(lambda p: unit(place(3, 1), 3, 3, p))
    rims(place(3, 1))
    k_arrive(3, 1, 0)
    unit(place(3, 3), 3, 1, 0)
    unit(CROSS + 3, 3, 1, 0)
    d_arrive(CROSS + 2)
    cross_block(2)

    d_arrive(place(3, 0))
    d_copy(3, 0).start()
    both(lambda p: unit(place(3, 0), 3, 3, p))
    rims(place(3, 0))
    for c in (1, 0):
        k_arrive(2, c, 1)
        k_copy(2, c, 1).start()
    unit(place(1, 1), 1, 0, 1)
    r_copy(place(1, 1), 1).start()
    d_arrive(CROSS + 1)
    cross_block(1)
    loop(2, lambda k: unit(place(2, 2), 2, k, 1))
    r_copy(place(2, 2), 1).start()

    k_arrive(3, 0, 0)
    unit(place(3, 3), 3, 0, 0)
    r_copy(place(3, 3), 0).start()
    d_arrive(CROSS)
    cross_block(0)

    def last_keys(c):
        unit(CROSS + c, LAST, 0, 0)
        r_copy(CROSS + c, 0).start()

    def leave(c):
        add_rim(CROSS + c, 0)
        o_cross(c, 0).start()

    def middle_keys(k):
        unit(place(3, 3), 3, k, 1)
        loop(DEPTHS, lambda c: unit(CROSS + c, LAST, k, 1))

    def pass_on(r, p):
        for c in range(r):
            add_rim(place(r, c), p)
            if p == 0:
                add_part(place(r, c), p)
                o_copy(r, c, p).start()
            else:
                def half(h):
                    add_part(place(r, c), p, h)
                    o_copy(r, c, p, h).start()
                loop(2, half)

    loop(DEPTHS, last_keys)
    loop(DEPTHS, leave)
    k_arrive(3, 2, 1)
    middle_keys(2)
    pass_on(3, 0)
    k_arrive(3, 1, 1)
    middle_keys(1)

    k_arrive(3, 0, 1)

    def last_half(i):
        c, h = i // 2, lax.rem(i, 2)
        unit(CROSS + c, LAST, 0, 1, h)
        r_copy(CROSS + c, 1, h).start()
    loop(2 * DEPTHS, last_half)
    unit(place(3, 3), 3, 0, 1)
    r_copy(place(3, 3), 1).start()

    def leave_half(i):
        c, h = i // 2, lax.rem(i, 2)
        add_rim(CROSS + c, 1, h)
        o_cross(c, 1, h).start()
    loop(2 * DEPTHS, leave_half)
    pass_on(2, 0)

    def finish(r, p):
        s = place(r, r)
        add_rim(s, p)
        if p == 0:
            add_part(s, p)
        else:
            loop(2, lambda h: add_part(s, p, h))
        first = lax.rem(quarter(r), 2) == 0
        mine = low == first

        def one(ct):
            v = main[s, p, ct]
            a = jnp.where(first, v, swap(v))
            b = jnp.where(first, swap(v), v)
            out[ct, p, tile(r), :WIDE] = jnp.where(mine, a, out[ct, p, tile(r), :WIDE])
            out[ct, p, tile(r), WIDE:] = jnp.where(mine, b, out[ct, p, tile(r), WIDE:])
        loop(cts, one)

    pass_on(3, 1)
    pass_on(1, 0)
    for r in (3, 2, 1):
        finish(r, 0)
    pass_on(2, 1)
    finish(0, 0)
    finish(3, 1)
    pass_on(1, 1)
    for r in (2, 1, 0):
        finish(r, 1)

    def sent(copy):
        copy(0).wait_send()
        loop(2, lambda h: copy(1, h).wait_send())

    for r in range(DEPTHS):
        for c in range(r + 1):
            d_copy(r, c).wait_send()
            if r < LAST:
                both(lambda p: k_copy(r, c, p).wait_send())
            if c < r:
                sent(lambda *ph: o_copy(r, c, *ph))
    for c in range(DEPTHS):
        sent(lambda *ph: o_cross(c, *ph))
        sent(lambda *ph: r_copy(CROSS + c, *ph))
    loop(2 * CROSS, lambda i: r_copy(i // 2, lax.rem(i, 2)).wait_send())


def per_device(digits, keys, requests, rotations, moduli):
    groups, limbs = lax.axis_size("grp"), lax.axis_size("limb")
    cts, dnum, limb_count, columns = digits.shape
    nkeys = keys.shape[0]
    modulus = moduli.astype(jnp.float32)
    f32 = jnp.float32
    dma = pltpu.SemaphoreType.DMA
    smem = pl.BlockSpec(memory_space=pltpu.SMEM)
    vmem = pl.BlockSpec(memory_space=pltpu.VMEM)
    any_space = pl.BlockSpec(memory_space=pl.ANY)
    rows = 2 * LIMBS
    total = pl.pallas_call(
        lambda *refs: kernel(groups, limbs, *refs),
        out_shape=jax.ShapeDtypeStruct((cts, 2, limb_count, columns), f32),
        in_specs=[smem, smem, any_space, any_space, vmem],
        out_specs=vmem,
        scratch_shapes=[
            pltpu.VMEM(digits.shape, f32),
            pltpu.VMEM(keys.shape, f32),
            pltpu.VMEM((2 * DEPTHS, rows, 128), f32),
            pltpu.VMEM((rows, 128), f32),
            pltpu.VMEM((SLOTS, cts * dnum + 1, rows, WIDE), f32),
            pltpu.VMEM((CROSS, 2, nkeys, dnum, rows, WIDE), f32),
            pltpu.VMEM((SLOTS, 2, cts, rows, WIDE), f32),
            pltpu.VMEM((CROSS, 2, cts, rows, WIDE), f32),
            pltpu.VMEM((SLOTS, 2, cts // 2, rows, WIDE), f32),
            pltpu.VMEM((SLOTS, 2, cts // 2, rows, WIDE), f32),
            dma((CROSS,)), dma((SLOTS,)),
            dma((CROSS, 2)), dma((CROSS, 2)),
            dma((SLOTS, 2, 2)), dma((CROSS, 2, 2)),
            dma((SLOTS, 2, 2)), dma((SLOTS, 2, 2)),
            dma((2,)),
        ],
        compiler_params=pltpu.CompilerParams(
            collective_id=0, has_side_effects=True, vmem_limit_bytes=60 * 1024 * 1024),
        name="keyswitch",
    )(rotations, moduli, digits, keys, requests)
    column = modulus[:, None]
    return reduce_mod(total, column) / column


def solution(mesh):
    in_specs = (
        P("grp", None, None, "limb"),
        P("grp", None, None, None, "limb"),
        P("grp", None),
        P(),
        P(),
    )
    out_specs = P("grp", None, None, "limb")
    return jax.shard_map(
        per_device, mesh=mesh, in_specs=in_specs, out_specs=out_specs, check_vma=False
    )
```

```python
import jax
import jax.numpy as jnp
from jax import lax
from jax.experimental import pallas as pl
from jax.experimental.pallas import tpu as pltpu
from jax.sharding import PartitionSpec as P

MESH = pl.DeviceIdType.MESH
WIDE = 512
DEPTHS = 4
LIMBS = 4


def reduce_mod(amount, modulus):
    quotient = jnp.floor(amount * (1.0 / modulus))
    remainder = amount - quotient * modulus
    remainder = jnp.where(remainder < 0, remainder + modulus, remainder)
    return jnp.where(remainder >= modulus, remainder - modulus, remainder)


def place(r, c):
    return r * (r + 1) // 2 + c


CROSS = place(DEPTHS, 0)
SLOTS = CROSS + DEPTHS
LAST = DEPTHS - 1


def kernel(groups, limbs, rot, mods, digits, keys, requests, out,
           stage_d, stage_k, consts, flag, dbuf, kbuf, main, part_in, rim_out, rim_in,
           d_send, d_recv, k_send, k_recv, o_send, o_recv, r_send, r_recv, local):
    z = lax.axis_index("grp")
    lb = lax.axis_index("limb")
    before = lax.rem(lb + limbs - 1, limbs)
    after = lax.rem(lb + 1, limbs)
    cts, dnum = digits.shape[:2]
    nkeys = keys.shape[0]
    pages = cts * dnum
    rows = 2 * LIMBS
    f32 = jnp.float32

    def zmod(value):
        return lax.rem(value, groups)

    def side(r):
        return lax.rem(z + r, 2)

    def inward(r):
        return zmod(z + 1 + (groups - 2) * side(r))

    def outward(r):
        return zmod(z + groups - 1 + 2 * side(r))

    def quarter(r):
        at = r * (1 - side(r)) + (groups - 1 - r) * side(r)
        return zmod(at + groups - z) // 2

    sub = lax.broadcasted_iota(jnp.int32, (rows, WIDE), 0)
    lane = lax.broadcasted_iota(jnp.int32, (rows, WIDE), 1)
    low = sub < LIMBS

    def swap(x):
        return pltpu.roll(x, LIMBS, 0)

    def remote(src, dst, send, recv, zt, lt):
        return pltpu.make_async_remote_copy(
            src_ref=src, dst_ref=dst, send_sem=send, recv_sem=recv,
            device_id=(zt, lt), device_id_type=MESH)

    def d_copy(r, c):
        s = place(r, c)
        t = place(r + 1, c) if r < LAST else CROSS + c
        return remote(dbuf.at[s], dbuf.at[t], d_send.at[s], d_recv.at[t], inward(r), lb)

    def d_arrive(t):
        remote(dbuf.at[t], dbuf.at[t], d_send.at[0], d_recv.at[t], z, lb).wait_recv()

    def k_copy(r, c, p):
        s, t = place(r, c), place(r + 1, c)
        return remote(kbuf.at[s, p], kbuf.at[t, p], k_send.at[s, p], k_recv.at[t, p],
                      inward(r), lb)

    def k_arrive(r, c, p):
        t = place(r, c)
        remote(kbuf.at[t, p], kbuf.at[t, p], k_send.at[0, p], k_recv.at[t, p], z, lb).wait_recv()

    def view(ref, s, p, h):
        return ref.at[s, p] if h is None else ref.at[s, p, pl.ds(2 * h, 2)]

    def o_cross(c, p, h=None):
        s, t, e = CROSS + c, place(LAST, c), 0 if h is None else h
        return remote(view(main, s, p, h), view(part_in, t, p, h),
                      o_send.at[s, p, e], o_recv.at[t, p, e], inward(LAST), lb)

    def o_copy(r, c, p, h=None):
        s, t, e = place(r, c), place(r - 1, c), 0 if h is None else h
        return remote(view(main, s, p, h), view(part_in, t, p, h),
                      o_send.at[s, p, e], o_recv.at[t, p, e], outward(r), lb)

    def r_copy(s, p, h=None):
        e = 0 if h is None else h
        src, dst = rim_out.at[s, p], rim_in.at[s, p]
        if h is not None:
            src, dst = src.at[pl.ds(h, 1)], dst.at[pl.ds(h, 1)]
        return remote(src, dst, r_send.at[s, p, e], r_recv.at[s, p, e], z, before)

    def loop(count, body):
        lax.fori_loop(0, count, lambda i, c: (body(i), c)[1], 0)

    def tiled(x):
        return jnp.concatenate([x] * (WIDE // 128), axis=1)

    def unit(s, r, k, p, h=None):
        held = r * (r + 1) // 2 + k
        zk = zmod(z + groups + (k - r) * (1 - 2 * side(r)))
        m = tiled(consts[r])
        inv = tiled(consts[DEPTHS + r])

        def pair(h):
            flags = pltpu.roll(dbuf[s, pages, :, :128],
                               lax.rem(256 - 64 * h - nkeys * zk, 128), 1)
            rim = rim_out[s, p, h]
            for e in range(2):
                ct = 2 * h + e
                total = jnp.zeros((rows, WIDE), f32)
                inside = jnp.zeros((rows, WIDE), f32)
                for key in range(nkeys):
                    x = dbuf[s, dnum * ct] * kbuf[held, p, key, 0]
                    for j in range(1, dnum):
                        x = x + dbuf[s, dnum * ct + j] * kbuf[held, p, key, j]
                    wanted = flags[:, 32 * e + key:32 * e + key + 1]
                    t = (x - jnp.floor(x * inv) * m) * wanted
                    kept = WIDE - 2 * rot[nkeys * zk + key]
                    t = pltpu.roll(t, kept, 1)
                    total = total + t
                    inside = inside + jnp.where(lane < kept, t, 0.0)
                wrapped = total - inside
                turned = swap(wrapped)
                main[s, p, ct] = main[s, p, ct] + (inside + jnp.where(low, turned, 0.0))
                if e == 0:
                    rim = rim + jnp.where(low, 0.0, turned)
                else:
                    rim = rim + jnp.where(low, wrapped, 0.0)
            rim_out[s, p, h] = rim
        if h is None:
            loop(cts // 2, pair)
        else:
            pair(h)

    def both(body):
        loop(2, body)

    def rims(s):
        both(lambda p: r_copy(s, p).start())

    def add_rim(s, p, h=None):
        r_copy(s, p, h).wait_recv()

        def pair(h):
            rim = rim_in[s, p, h]
            main[s, p, 2 * h] = main[s, p, 2 * h] + jnp.where(low, 0.0, rim)
            main[s, p, 2 * h + 1] = main[s, p, 2 * h + 1] + jnp.where(low, 0.0, swap(rim))
        if h is None:
            loop(cts // 2, pair)
        else:
            pair(h)

    def add_part(s, p, h=None):
        whole = view(part_in, s, p, h)
        e = 0 if h is None else h
        remote(whole, whole, o_send.at[0, p, e], o_recv.at[s, p, e], z, lb).wait_recv()
        at = (s, p) if h is None else (s, p, pl.ds(2 * h, 2))
        main[at] = main[at] + part_in[at]

    copy_d = pltpu.make_async_copy(digits, stage_d, local.at[0])
    copy_k = pltpu.make_async_copy(keys, stage_k, local.at[1])
    copy_d.start()
    copy_k.start()
    barrier = pltpu.get_barrier_semaphore()
    for zt, lt in ((zmod(z + 1), lb), (zmod(z + groups - 1), lb), (z, before), (z, after)):
        pl.semaphore_signal(barrier, inc=1, device_id=(zt, lt), device_id_type=MESH)

    row = lax.broadcasted_iota(jnp.int32, (rows, 128), 0)
    flag[...] = jnp.zeros_like(flag)
    flag[:cts, :requests.shape[1]] = requests[...].astype(f32)
    wanted = jnp.zeros((rows, 128), f32)
    for ct in range(cts):
        wanted = wanted + pltpu.roll(jnp.broadcast_to(flag[ct:ct + 1, :], (rows, 128)), 32 * ct, 1)
    wanted = jnp.concatenate([wanted] + [jnp.zeros((rows, 128), f32)] * (WIDE // 128 - 1), axis=1)
    for r in range(DEPTHS):
        dbuf[place(r, r), pages] = wanted
        m = jnp.ones((rows, 128), f32)
        for limb in range(LIMBS):
            value = mods[LIMBS * quarter(r) + limb].astype(f32)
            m = jnp.where((row == limb) | (row == limb + LIMBS), value, m)
        consts[r] = m
        consts[DEPTHS + r] = 1.0 / m

    def folded(x, r):
        first = lax.rem(quarter(r), 2) == 0
        a, b = x[:, :WIDE], x[:, WIDE:]
        return jnp.where(low, jnp.where(first, a, swap(a)), jnp.where(first, swap(b), b))

    def tile(r):
        return pl.ds(pl.multiple_of(rows * (quarter(r) // 2), rows), rows)

    copy_d.wait()
    for r in range(DEPTHS):
        def fold_d(i):
            dbuf[place(r, r), i] = folded(stage_d[i // dnum, lax.rem(i, dnum), tile(r), :], r)
        loop(pages, fold_d)
    pl.semaphore_wait(barrier, 4)
    for r in (0, 1, 2, 3):
        d_copy(r, r).start()
    copy_k.wait()

    def fold_keys(r, p):
        def fold_k(i):
            key, j = i // dnum, lax.rem(i, dnum)
            kbuf[place(r, r), p, key, j] = folded(stage_k[key, j, p, tile(r), :], r)
        loop(nkeys * dnum, fold_k)
    fold_keys(0, 0)
    k_copy(0, 0, 0).start()
    for r, p in ((1, 0), (2, 0), (3, 0), (0, 1), (1, 1), (2, 1), (3, 1)):
        fold_keys(r, p)

    def clear(i):
        s, p = i // 2, lax.rem(i, 2)
        main[s, p] = jnp.zeros(main.shape[2:], f32)
        rim_out[s, p] = jnp.zeros(rim_out.shape[2:], f32)
    loop(2 * SLOTS, clear)

    def own(i):
        r, p = i // 2, lax.rem(i, 2)
        unit(r * (r + 3) // 2, r, r, p)
    loop(2 * DEPTHS, own)
    rims(place(0, 0))

    def from_next(i, r0):
        r, p = r0 + i // 2, lax.rem(i, 2)
        unit(r * (r + 1) // 2 + r - 1, r, r, p)

    def block(s):
        both(lambda p: unit(s, LAST, LAST, p))
        rims(s)

    d_arrive(place(1, 0))
    d_copy(1, 0).start()
    k_copy(1, 1, 0).start()
    d_arrive(place(2, 1))
    d_copy(2, 1).start()
    loop(4, lambda i: from_next(i, 1))
    rims(place(1, 0))
    rims(place(2, 1))
    d_arrive(place(3, 2))
    d_copy(3, 2).start()
    block(place(3, 2))
    k_arrive(1, 0, 0)
    k_copy(1, 0, 0).start()
    d_arrive(place(2, 0))
    d_copy(2, 0).start()
    k_copy(2, 2, 0).start()
    d_arrive(CROSS + 3)
    both(lambda p: unit(CROSS + 3, LAST, LAST, p))
    both(lambda p: unit(place(2, 0), 2, 2, p))
    rims(place(2, 0))
    k_arrive(2, 1, 0)
    k_copy(2, 1, 0).start()
    d_arrive(place(3, 1))
    d_copy(3, 1).start()
    block(place(3, 1))
    d_arrive(CROSS + 2)
    both(lambda p: unit(CROSS + 2, LAST, LAST, p))
    d_arrive(place(3, 0))
    d_copy(3, 0).start()
    block(place(3, 0))
    k_arrive(2, 0, 0)
    k_copy(2, 0, 0).start()
    for r in (0, 1, 2):
        k_copy(r, r, 1).start()
    unit(place(1, 1), 1, 0, 0)
    r_copy(place(1, 1), 0).start()
    loop(2, lambda k: unit(place(2, 2), 2, k, 0))
    r_copy(place(2, 2), 0).start()
    for k in (2, 1):
        k_arrive(3, k, 0)
        unit(place(3, 3), LAST, k, 0)
        loop(2, lambda c: unit(CROSS + 2 + c, LAST, k, 0))

    def cross_block(c):
        loop(3, lambda i: unit(CROSS + c, LAST, LAST - i, 0))
        unit(CROSS + c, LAST, LAST, 1)
    for c in (1, 0):
        d_arrive(CROSS + c)
        cross_block(c)
    k_arrive(3, 0, 0)
    unit(place(3, 3), LAST, 0, 0)
    r_copy(place(3, 3), 0).start()

    def last_keys(c):
        unit(CROSS + c, LAST, 0, 0)
        r_copy(CROSS + c, 0).start()

    def leave(c):
        add_rim(CROSS + c, 0)
        o_cross(c, 0).start()

    def middle_keys(k):
        unit(place(3, 3), 3, k, 1)
        loop(DEPTHS, lambda c: unit(CROSS + c, LAST, k, 1))

    def pass_on(r, c, p):
        add_rim(place(r, c), p)
        if p == 0:
            add_part(place(r, c), p)
            o_copy(r, c, p).start()
        else:
            def half(h):
                add_part(place(r, c), p, h)
                o_copy(r, c, p, h).start()
            loop(2, half)

    loop(DEPTHS, last_keys)
    k_arrive(1, 0, 1)
    k_copy(1, 0, 1).start()
    unit(place(1, 1), 1, 0, 1)
    r_copy(place(1, 1), 1).start()
    k_arrive(2, 1, 1)
    k_copy(2, 1, 1).start()
    loop(DEPTHS, leave)
    unit(place(2, 2), 2, 1, 1)
    k_arrive(2, 0, 1)
    k_copy(2, 0, 1).start()
    unit(place(2, 2), 2, 0, 1)
    r_copy(place(2, 2), 1).start()
    k_arrive(3, 2, 1)
    middle_keys(2)
    for c in range(LAST):
        pass_on(3, c, 0)
    k_arrive(3, 1, 1)
    middle_keys(1)

    k_arrive(3, 0, 1)

    def last_half(i):
        c, h = i // 2, lax.rem(i, 2)
        unit(CROSS + c, LAST, 0, 1, h)
        r_copy(CROSS + c, 1, h).start()
    loop(2 * DEPTHS, last_half)
    unit(place(3, 3), 3, 0, 1)
    r_copy(place(3, 3), 1).start()

    def leave_half(i):
        c, h = i // 2, lax.rem(i, 2)
        add_rim(CROSS + c, 1, h)
        o_cross(c, 1, h).start()

    def finish(r, p):
        s = place(r, r)
        add_rim(s, p)
        if p == 0:
            add_part(s, p)
        else:
            loop(2, lambda h: add_part(s, p, h))
        first = lax.rem(quarter(r), 2) == 0
        mine = low == first

        def one(ct):
            v = main[s, p, ct]
            a = jnp.where(first, v, swap(v))
            b = jnp.where(first, swap(v), v)
            out[ct, p, tile(r), :WIDE] = jnp.where(mine, a, out[ct, p, tile(r), :WIDE])
            out[ct, p, tile(r), WIDE:] = jnp.where(mine, b, out[ct, p, tile(r), WIDE:])
        loop(cts, one)

    pass_on(2, 0, 0)
    loop(2, leave_half)
    pass_on(2, 1, 0)
    loop(2 * DEPTHS - 2, lambda i: leave_half(2 + i))
    pass_on(3, 0, 1)
    finish(3, 0)
    pass_on(1, 0, 0)
    pass_on(3, 1, 1)
    finish(2, 0)
    pass_on(2, 0, 1)
    pass_on(3, 2, 1)
    finish(1, 0)
    pass_on(2, 1, 1)
    pass_on(1, 0, 1)
    finish(0, 0)
    for r in (3, 2, 1, 0):
        finish(r, 1)

    def sent(copy):
        copy(0).wait_send()
        loop(2, lambda h: copy(1, h).wait_send())

    for r in range(DEPTHS):
        for c in range(r + 1):
            d_copy(r, c).wait_send()
            if r < LAST:
                both(lambda p: k_copy(r, c, p).wait_send())
            if c < r:
                sent(lambda *ph: o_copy(r, c, *ph))
    for c in range(DEPTHS):
        sent(lambda *ph: o_cross(c, *ph))
        sent(lambda *ph: r_copy(CROSS + c, *ph))
    loop(2 * CROSS, lambda i: r_copy(i // 2, lax.rem(i, 2)).wait_send())


def per_device(digits, keys, requests, rotations, moduli):
    groups, limbs = lax.axis_size("grp"), lax.axis_size("limb")
    cts, dnum, limb_count, columns = digits.shape
    nkeys = keys.shape[0]
    modulus = moduli.astype(jnp.float32)
    f32 = jnp.float32
    dma = pltpu.SemaphoreType.DMA
    smem = pl.BlockSpec(memory_space=pltpu.SMEM)
    vmem = pl.BlockSpec(memory_space=pltpu.VMEM)
    any_space = pl.BlockSpec(memory_space=pl.ANY)
    rows = 2 * LIMBS
    total = pl.pallas_call(
        lambda *refs: kernel(groups, limbs, *refs),
        out_shape=jax.ShapeDtypeStruct((cts, 2, limb_count, columns), f32),
        in_specs=[smem, smem, any_space, any_space, vmem],
        out_specs=vmem,
        scratch_shapes=[
            pltpu.VMEM(digits.shape, f32),
            pltpu.VMEM(keys.shape, f32),
            pltpu.VMEM((2 * DEPTHS, rows, 128), f32),
            pltpu.VMEM((rows, 128), f32),
            pltpu.VMEM((SLOTS, cts * dnum + 1, rows, WIDE), f32),
            pltpu.VMEM((CROSS, 2, nkeys, dnum, rows, WIDE), f32),
            pltpu.VMEM((SLOTS, 2, cts, rows, WIDE), f32),
            pltpu.VMEM((CROSS, 2, cts, rows, WIDE), f32),
            pltpu.VMEM((SLOTS, 2, cts // 2, rows, WIDE), f32),
            pltpu.VMEM((SLOTS, 2, cts // 2, rows, WIDE), f32),
            dma((CROSS,)), dma((SLOTS,)),
            dma((CROSS, 2)), dma((CROSS, 2)),
            dma((SLOTS, 2, 2)), dma((CROSS, 2, 2)),
            dma((SLOTS, 2, 2)), dma((SLOTS, 2, 2)),
            dma((2,)),
        ],
        compiler_params=pltpu.CompilerParams(
            collective_id=0, has_side_effects=True, vmem_limit_bytes=60 * 1024 * 1024),
        name="keyswitch",
    )(rotations, moduli, digits, keys, requests)
    column = modulus[:, None]
    return reduce_mod(total, column) / column


def solution(mesh):
    in_specs = (
        P("grp", None, None, "limb"),
        P("grp", None, None, None, "limb"),
        P("grp", None),
        P(),
        P(),
    )
    out_specs = P("grp", None, None, "limb")
    return jax.shard_map(
        per_device, mesh=mesh, in_specs=in_specs, out_specs=out_specs, check_vma=False
    )
```

```python
import jax
import jax.numpy as jnp
from jax import lax
from jax.experimental import pallas as pl
from jax.experimental.pallas import tpu as pltpu
from jax.sharding import PartitionSpec as P

MESH = pl.DeviceIdType.MESH
WIDE = 512
DEPTHS = 4
LIMBS = 4


def place(r, c):
    return r * (r + 1) // 2 + c


CROSS = place(DEPTHS, 0)
SLOTS = CROSS + DEPTHS
LAST = DEPTHS - 1


def kernel(groups, limbs, rot, mods, digits, keys, requests, out,
           stage_d, stage_k, consts, flag, dbuf, kbuf, main, part_in, rim_out, rim_in,
           d_send, d_recv, k_send, k_recv, o_send, o_recv, r_send, r_recv, local):
    z = lax.axis_index("grp")
    lb = lax.axis_index("limb")
    before = lax.rem(lb + limbs - 1, limbs)
    after = lax.rem(lb + 1, limbs)
    cts, dnum = digits.shape[:2]
    nkeys = keys.shape[0]
    pages = cts * dnum
    rows = 2 * LIMBS
    f32 = jnp.float32

    def zmod(value):
        return lax.rem(value, groups)

    def side(r):
        return lax.rem(z + r, 2)

    def inward(r):
        return zmod(z + 1 + (groups - 2) * side(r))

    def outward(r):
        return zmod(z + groups - 1 + 2 * side(r))

    def quarter(r):
        at = r * (1 - side(r)) + (groups - 1 - r) * side(r)
        return zmod(at + groups - z) // 2

    sub = lax.broadcasted_iota(jnp.int32, (rows, WIDE), 0)
    lane = lax.broadcasted_iota(jnp.int32, (rows, WIDE), 1)
    low = sub < LIMBS

    def swap(x):
        return pltpu.roll(x, LIMBS, 0)

    def remote(src, dst, send, recv, zt, lt):
        return pltpu.make_async_remote_copy(
            src_ref=src, dst_ref=dst, send_sem=send, recv_sem=recv,
            device_id=(zt, lt), device_id_type=MESH)

    def d_copy(r, c):
        s = place(r, c)
        t = place(r + 1, c) if r < LAST else CROSS + c
        return remote(dbuf.at[s], dbuf.at[t], d_send.at[s], d_recv.at[t], inward(r), lb)

    def d_arrive(t):
        remote(dbuf.at[t], dbuf.at[t], d_send.at[0], d_recv.at[t], z, lb).wait_recv()

    def k_copy(r, c, p):
        s, t = place(r, c), place(r + 1, c)
        return remote(kbuf.at[s, p], kbuf.at[t, p], k_send.at[s, p], k_recv.at[t, p],
                      inward(r), lb)

    def k_arrive(r, c, p):
        t = place(r, c)
        remote(kbuf.at[t, p], kbuf.at[t, p], k_send.at[0, p], k_recv.at[t, p], z, lb).wait_recv()

    def view(ref, s, p, h):
        return ref.at[s, p] if h is None else ref.at[s, p, pl.ds(2 * h, 2)]

    def o_cross(c, p, h=None):
        s, t, e = CROSS + c, place(LAST, c), 0 if h is None else h
        return remote(view(main, s, p, h), view(part_in, t, p, h),
                      o_send.at[s, p, e], o_recv.at[t, p, e], inward(LAST), lb)

    def o_copy(r, c, p, h=None):
        s, t, e = place(r, c), place(r - 1, c), 0 if h is None else h
        return remote(view(main, s, p, h), view(part_in, t, p, h),
                      o_send.at[s, p, e], o_recv.at[t, p, e], outward(r), lb)

    def r_copy(s, p, h=None):
        e = 0 if h is None else h
        src, dst = rim_out.at[s, p], rim_in.at[s, p]
        if h is not None:
            src, dst = src.at[pl.ds(h, 1)], dst.at[pl.ds(h, 1)]
        return remote(src, dst, r_send.at[s, p, e], r_recv.at[s, p, e], z, before)

    def loop(count, body):
        lax.fori_loop(0, count, lambda i, c: (body(i), c)[1], 0)

    def tiled(x):
        return jnp.concatenate([x] * (WIDE // 128), axis=1)

    def unit(s, r, k, p, h=None):
        held = r * (r + 1) // 2 + k
        zk = zmod(z + groups + (k - r) * (1 - 2 * side(r)))
        m = tiled(consts[r])
        inv = tiled(consts[DEPTHS + r])

        def pair(h):
            flags = pltpu.roll(dbuf[s, pages, :, :128],
                               lax.rem(256 - 64 * h - nkeys * zk, 128), 1)
            rim = rim_out[s, p, h]
            for e in range(2):
                ct = 2 * h + e
                total = jnp.zeros((rows, WIDE), f32)
                inside = jnp.zeros((rows, WIDE), f32)
                for key in range(nkeys):
                    x = dbuf[s, dnum * ct] * kbuf[held, p, key, 0]
                    for j in range(1, dnum):
                        x = x + dbuf[s, dnum * ct + j] * kbuf[held, p, key, j]
                    wanted = flags[:, 32 * e + key:32 * e + key + 1]
                    t = (x - jnp.floor(x * inv) * m) * wanted
                    kept = WIDE - 2 * rot[nkeys * zk + key]
                    t = pltpu.roll(t, kept, 1)
                    total = total + t
                    inside = inside + jnp.where(lane < kept, t, 0.0)
                wrapped = total - inside
                turned = swap(wrapped)
                main[s, p, ct] = main[s, p, ct] + (inside + jnp.where(low, turned, 0.0))
                if e == 0:
                    rim = rim + jnp.where(low, 0.0, turned)
                else:
                    rim = rim + jnp.where(low, wrapped, 0.0)
            rim_out[s, p, h] = rim
        if h is None:
            loop(cts // 2, pair)
        else:
            pair(h)

    def both(body):
        loop(2, body)

    def rims(s):
        both(lambda p: r_copy(s, p).start())

    def add_rim(s, p, h=None):
        r_copy(s, p, h).wait_recv()

        def pair(h):
            rim = rim_in[s, p, h]
            main[s, p, 2 * h] = main[s, p, 2 * h] + jnp.where(low, 0.0, rim)
            main[s, p, 2 * h + 1] = main[s, p, 2 * h + 1] + jnp.where(low, 0.0, swap(rim))
        if h is None:
            loop(cts // 2, pair)
        else:
            pair(h)

    def add_part(s, p, h=None):
        whole = view(part_in, s, p, h)
        e = 0 if h is None else h
        remote(whole, whole, o_send.at[0, p, e], o_recv.at[s, p, e], z, lb).wait_recv()
        at = (s, p) if h is None else (s, p, pl.ds(2 * h, 2))
        main[at] = main[at] + part_in[at]

    copy_d = pltpu.make_async_copy(digits, stage_d, local.at[0])
    copy_k = pltpu.make_async_copy(keys, stage_k, local.at[1])
    copy_d.start()
    copy_k.start()
    barrier = pltpu.get_barrier_semaphore()
    for zt, lt in ((zmod(z + 1), lb), (zmod(z + groups - 1), lb), (z, before), (z, after)):
        pl.semaphore_signal(barrier, inc=1, device_id=(zt, lt), device_id_type=MESH)

    row = lax.broadcasted_iota(jnp.int32, (rows, 128), 0)
    flag[...] = jnp.zeros_like(flag)
    flag[:cts, :requests.shape[1]] = requests[...].astype(f32)
    wanted = jnp.zeros((rows, 128), f32)
    for ct in range(cts):
        wanted = wanted + pltpu.roll(jnp.broadcast_to(flag[ct:ct + 1, :], (rows, 128)), 32 * ct, 1)
    wanted = jnp.concatenate([wanted] + [jnp.zeros((rows, 128), f32)] * (WIDE // 128 - 1), axis=1)
    for r in range(DEPTHS):
        dbuf[place(r, r), pages] = wanted
        m = jnp.ones((rows, 128), f32)
        for limb in range(LIMBS):
            value = mods[LIMBS * quarter(r) + limb].astype(f32)
            m = jnp.where((row == limb) | (row == limb + LIMBS), value, m)
        consts[r] = m
        consts[DEPTHS + r] = 1.0 / m

    def folded(x, r):
        first = lax.rem(quarter(r), 2) == 0
        a, b = x[:, :WIDE], x[:, WIDE:]
        return jnp.where(low, jnp.where(first, a, swap(a)), jnp.where(first, swap(b), b))

    def tile(r):
        return pl.ds(pl.multiple_of(rows * (quarter(r) // 2), rows), rows)

    copy_d.wait()
    pl.semaphore_wait(barrier, 4)
    for r in range(DEPTHS):
        def fold_d(ct):
            for j in range(dnum):
                dbuf[place(r, r), dnum * ct + j] = folded(stage_d[ct, j, tile(r), :], r)
        loop(cts, fold_d)
        d_copy(r, r).start()
    copy_k.wait()

    def fold_keys(r, p):
        def fold_k(key):
            for j in range(dnum):
                kbuf[place(r, r), p, key, j] = folded(stage_k[key, j, p, tile(r), :], r)
        loop(nkeys, fold_k)
    fold_keys(0, 0)
    k_copy(0, 0, 0).start()
    for r, p in ((1, 0), (2, 0), (3, 0), (0, 1), (1, 1), (2, 1), (3, 1)):
        fold_keys(r, p)

    def clear(i):
        s, p = i // 2, lax.rem(i, 2)
        main[s, p] = jnp.zeros(main.shape[2:], f32)
        rim_out[s, p] = jnp.zeros(rim_out.shape[2:], f32)
    loop(2 * SLOTS, clear)

    def own(i):
        r, p = i // 2, lax.rem(i, 2)
        unit(r * (r + 3) // 2, r, r, p)
    loop(2 * DEPTHS, own)
    rims(place(0, 0))

    def from_next(i, r0):
        r, p = r0 + i // 2, lax.rem(i, 2)
        unit(r * (r + 1) // 2 + r - 1, r, r, p)

    def block(s):
        both(lambda p: unit(s, LAST, LAST, p))
        rims(s)

    d_arrive(place(1, 0))
    d_copy(1, 0).start()
    k_copy(1, 1, 0).start()
    d_arrive(place(2, 1))
    d_copy(2, 1).start()
    loop(4, lambda i: from_next(i, 1))
    rims(place(1, 0))
    rims(place(2, 1))
    d_arrive(place(3, 2))
    d_copy(3, 2).start()
    block(place(3, 2))
    k_arrive(1, 0, 0)
    k_copy(1, 0, 0).start()
    d_arrive(place(2, 0))
    d_copy(2, 0).start()
    k_copy(2, 2, 0).start()
    d_arrive(CROSS + 3)
    both(lambda p: unit(CROSS + 3, LAST, LAST, p))
    both(lambda p: unit(place(2, 0), 2, 2, p))
    rims(place(2, 0))
    k_arrive(2, 1, 0)
    k_copy(2, 1, 0).start()
    d_arrive(place(3, 1))
    d_copy(3, 1).start()
    block(place(3, 1))
    d_arrive(CROSS + 2)
    both(lambda p: unit(CROSS + 2, LAST, LAST, p))
    d_arrive(place(3, 0))
    d_copy(3, 0).start()
    block(place(3, 0))
    k_arrive(2, 0, 0)
    k_copy(2, 0, 0).start()
    for r in (0, 1, 2):
        k_copy(r, r, 1).start()
    unit(place(1, 1), 1, 0, 0)
    r_copy(place(1, 1), 0).start()
    loop(2, lambda k: unit(place(2, 2), 2, k, 0))
    r_copy(place(2, 2), 0).start()
    for k in (2, 1):
        k_arrive(3, k, 0)
        unit(place(3, 3), LAST, k, 0)
        loop(2, lambda c: unit(CROSS + 2 + c, LAST, k, 0))

    def cross_block(c):
        loop(3, lambda i: unit(CROSS + c, LAST, LAST - i, 0))
        unit(CROSS + c, LAST, LAST, 1)
    for c in (1, 0):
        d_arrive(CROSS + c)
        cross_block(c)
    k_arrive(3, 0, 0)
    unit(place(3, 3), LAST, 0, 0)
    r_copy(place(3, 3), 0).start()

    def last_keys(c):
        unit(CROSS + c, LAST, 0, 0)
        r_copy(CROSS + c, 0).start()

    def leave(c):
        add_rim(CROSS + c, 0)
        o_cross(c, 0).start()

    def middle_keys(k):
        unit(place(3, 3), 3, k, 1)
        loop(DEPTHS, lambda c: unit(CROSS + c, LAST, k, 1))

    def pass_on(r, c, p):
        add_rim(place(r, c), p)
        if p == 0:
            add_part(place(r, c), p)
            o_copy(r, c, p).start()
        else:
            def half(h):
                add_part(place(r, c), p, h)
                o_copy(r, c, p, h).start()
            loop(2, half)

    loop(DEPTHS, last_keys)
    k_arrive(1, 0, 1)
    k_copy(1, 0, 1).start()
    unit(place(1, 1), 1, 0, 1)
    r_copy(place(1, 1), 1).start()
    k_arrive(2, 1, 1)
    k_copy(2, 1, 1).start()
    loop(DEPTHS, leave)
    unit(place(2, 2), 2, 1, 1)
    k_arrive(2, 0, 1)
    k_copy(2, 0, 1).start()
    unit(place(2, 2), 2, 0, 1)
    r_copy(place(2, 2), 1).start()
    k_arrive(3, 2, 1)
    middle_keys(2)
    for c in range(LAST):
        pass_on(3, c, 0)
    k_arrive(3, 1, 1)
    middle_keys(1)

    k_arrive(3, 0, 1)

    def last_half(i):
        c, h = i // 2, lax.rem(i, 2)
        unit(CROSS + c, LAST, 0, 1, h)
        r_copy(CROSS + c, 1, h).start()
    loop(2 * DEPTHS, last_half)
    unit(place(3, 3), 3, 0, 1)
    r_copy(place(3, 3), 1).start()

    def leave_half(i):
        c, h = i // 2, lax.rem(i, 2)
        add_rim(CROSS + c, 1, h)
        o_cross(c, 1, h).start()

    def finish(r, p):
        s = place(r, r)
        add_rim(s, p)
        if p == 0:
            add_part(s, p)
        else:
            loop(2, lambda h: add_part(s, p, h))
        first = lax.rem(quarter(r), 2) == 0
        mine = low == first
        m, inv = tiled(consts[r]), tiled(consts[DEPTHS + r])

        def one(ct):
            v = main[s, p, ct]
            v = v - jnp.floor(v * inv) * m
            v = jnp.where(v < 0, v + m, v)
            v = jnp.where(v >= m, v - m, v) / m
            a = jnp.where(first, v, swap(v))
            b = jnp.where(first, swap(v), v)
            out[ct, p, tile(r), :WIDE] = jnp.where(mine, a, out[ct, p, tile(r), :WIDE])
            out[ct, p, tile(r), WIDE:] = jnp.where(mine, b, out[ct, p, tile(r), WIDE:])
        loop(cts, one)

    pass_on(2, 0, 0)
    loop(2, leave_half)
    pass_on(2, 1, 0)
    loop(2 * DEPTHS - 2, lambda i: leave_half(2 + i))
    pass_on(3, 0, 1)
    finish(3, 0)
    pass_on(1, 0, 0)
    pass_on(3, 1, 1)
    finish(2, 0)
    pass_on(2, 0, 1)
    pass_on(3, 2, 1)
    finish(1, 0)
    pass_on(2, 1, 1)
    pass_on(1, 0, 1)
    finish(0, 0)
    for r in (3, 2, 1, 0):
        finish(r, 1)

    def sent(copy):
        copy(0).wait_send()
        loop(2, lambda h: copy(1, h).wait_send())

    for r in range(DEPTHS):
        for c in range(r + 1):
            d_copy(r, c).wait_send()
            if r < LAST:
                both(lambda p: k_copy(r, c, p).wait_send())
            if c < r:
                sent(lambda *ph: o_copy(r, c, *ph))
    for c in range(DEPTHS):
        sent(lambda *ph: o_cross(c, *ph))
        sent(lambda *ph: r_copy(CROSS + c, *ph))
    loop(2 * CROSS, lambda i: r_copy(i // 2, lax.rem(i, 2)).wait_send())


def per_device(digits, keys, requests, rotations, moduli):
    groups, limbs = lax.axis_size("grp"), lax.axis_size("limb")
    cts, dnum, limb_count, columns = digits.shape
    nkeys = keys.shape[0]
    f32 = jnp.float32
    dma = pltpu.SemaphoreType.DMA
    smem = pl.BlockSpec(memory_space=pltpu.SMEM)
    vmem = pl.BlockSpec(memory_space=pltpu.VMEM)
    any_space = pl.BlockSpec(memory_space=pl.ANY)
    rows = 2 * LIMBS
    return pl.pallas_call(
        lambda *refs: kernel(groups, limbs, *refs),
        out_shape=jax.ShapeDtypeStruct((cts, 2, limb_count, columns), f32),
        in_specs=[smem, smem, any_space, any_space, vmem],
        out_specs=vmem,
        scratch_shapes=[
            pltpu.VMEM(digits.shape, f32),
            pltpu.VMEM(keys.shape, f32),
            pltpu.VMEM((2 * DEPTHS, rows, 128), f32),
            pltpu.VMEM((rows, 128), f32),
            pltpu.VMEM((SLOTS, cts * dnum + 1, rows, WIDE), f32),
            pltpu.VMEM((CROSS, 2, nkeys, dnum, rows, WIDE), f32),
            pltpu.VMEM((SLOTS, 2, cts, rows, WIDE), f32),
            pltpu.VMEM((CROSS, 2, cts, rows, WIDE), f32),
            pltpu.VMEM((SLOTS, 2, cts // 2, rows, WIDE), f32),
            pltpu.VMEM((SLOTS, 2, cts // 2, rows, WIDE), f32),
            dma((CROSS,)), dma((SLOTS,)),
            dma((CROSS, 2)), dma((CROSS, 2)),
            dma((SLOTS, 2, 2)), dma((CROSS, 2, 2)),
            dma((SLOTS, 2, 2)), dma((SLOTS, 2, 2)),
            dma((2,)),
        ],
        compiler_params=pltpu.CompilerParams(
            collective_id=0, has_side_effects=True, vmem_limit_bytes=60 * 1024 * 1024),
        name="keyswitch",
    )(rotations, moduli, digits, keys, requests)


def solution(mesh):
    in_specs = (
        P("grp", None, None, "limb"),
        P("grp", None, None, None, "limb"),
        P("grp", None),
        P(),
        P(),
    )
    out_specs = P("grp", None, None, "limb")
    return jax.shard_map(
        per_device, mesh=mesh, in_specs=in_specs, out_specs=out_specs, check_vma=False
    )
```

```python
import jax
import jax.numpy as jnp
from jax import lax
from jax.experimental import pallas as pl
from jax.experimental.pallas import tpu as pltpu
from jax.sharding import PartitionSpec as P

MESH = pl.DeviceIdType.MESH
WIDE = 512
DEPTHS = 4
LIMBS = 4


def place(r, c):
    return r * (r + 1) // 2 + c


CROSS = place(DEPTHS, 0)
SLOTS = CROSS + DEPTHS
LAST = DEPTHS - 1


def kernel(groups, limbs, rot, mods, digits, keys, requests, out,
           stage_d, stage_k, consts, flag, dbuf, kbuf, main, part_in, rim_out, rim_in,
           d_send, d_recv, k_send, k_recv, o_send, o_recv, r_send, r_recv, local):
    z = lax.axis_index("grp")
    lb = lax.axis_index("limb")
    before = lax.rem(lb + limbs - 1, limbs)
    after = lax.rem(lb + 1, limbs)
    cts, dnum = digits.shape[:2]
    nkeys = keys.shape[0]
    pages = cts * dnum
    rows = 2 * LIMBS
    f32 = jnp.float32

    def zmod(value):
        return lax.rem(value, groups)

    def side(r):
        return lax.rem(z + r, 2)

    def inward(r):
        return zmod(z + 1 + (groups - 2) * side(r))

    def outward(r):
        return zmod(z + groups - 1 + 2 * side(r))

    def quarter(r):
        at = r * (1 - side(r)) + (groups - 1 - r) * side(r)
        return zmod(at + groups - z) // 2

    sub = lax.broadcasted_iota(jnp.int32, (rows, WIDE), 0)
    lane = lax.broadcasted_iota(jnp.int32, (rows, WIDE), 1)
    low = sub < LIMBS

    def swap(x):
        return pltpu.roll(x, LIMBS, 0)

    def remote(src, dst, send, recv, zt, lt):
        return pltpu.make_async_remote_copy(
            src_ref=src, dst_ref=dst, send_sem=send, recv_sem=recv,
            device_id=(zt, lt), device_id_type=MESH)

    def d_copy(r, c):
        s = place(r, c)
        t = place(r + 1, c) if r < LAST else CROSS + c
        return remote(dbuf.at[s], dbuf.at[t], d_send.at[s], d_recv.at[t], inward(r), lb)

    def d_arrive(t):
        remote(dbuf.at[t], dbuf.at[t], d_send.at[0], d_recv.at[t], z, lb).wait_recv()

    def k_copy(r, c, p):
        s, t = place(r, c), place(r + 1, c)
        return remote(kbuf.at[s, p], kbuf.at[t, p], k_send.at[s, p], k_recv.at[t, p],
                      inward(r), lb)

    def k_arrive(r, c, p):
        t = place(r, c)
        remote(kbuf.at[t, p], kbuf.at[t, p], k_send.at[0, p], k_recv.at[t, p], z, lb).wait_recv()

    def view(ref, s, p, h):
        return ref.at[s, p] if h is None else ref.at[s, p, pl.ds(2 * h, 2)]

    def o_cross(c, p, h=None):
        s, t, e = CROSS + c, place(LAST, c), 0 if h is None else h
        return remote(view(main, s, p, h), view(part_in, t, p, h),
                      o_send.at[s, p, e], o_recv.at[t, p, e], inward(LAST), lb)

    def o_copy(r, c, p, h=None):
        s, t, e = place(r, c), place(r - 1, c), 0 if h is None else h
        return remote(view(main, s, p, h), view(part_in, t, p, h),
                      o_send.at[s, p, e], o_recv.at[t, p, e], outward(r), lb)

    def r_copy(s, p, h=None):
        e = 0 if h is None else h
        src, dst = rim_out.at[s, p], rim_in.at[s, p]
        if h is not None:
            src, dst = src.at[pl.ds(h, 1)], dst.at[pl.ds(h, 1)]
        return remote(src, dst, r_send.at[s, p, e], r_recv.at[s, p, e], z, before)

    def loop(count, body):
        lax.fori_loop(0, count, lambda i, c: (body(i), c)[1], 0)

    def tiled(x):
        return jnp.concatenate([x] * (WIDE // 128), axis=1)

    def unit(s, r, k, p, h=None):
        held = r * (r + 1) // 2 + k
        zk = zmod(z + groups + (k - r) * (1 - 2 * side(r)))
        m = tiled(consts[r])
        inv = tiled(consts[DEPTHS + r])

        def pair(h):
            flags = pltpu.roll(dbuf[s, pages, :, :128],
                               lax.rem(256 - 64 * h - nkeys * zk, 128), 1)
            rim = rim_out[s, p, h]
            for e in range(2):
                ct = 2 * h + e
                total = jnp.zeros((rows, WIDE), f32)
                inside = jnp.zeros((rows, WIDE), f32)
                for key in range(nkeys):
                    x = dbuf[s, dnum * ct] * kbuf[held, p, key, 0]
                    for j in range(1, dnum):
                        x = x + dbuf[s, dnum * ct + j] * kbuf[held, p, key, j]
                    wanted = flags[:, 32 * e + key:32 * e + key + 1]
                    t = (x - jnp.floor(x * inv) * m) * wanted
                    kept = WIDE - 2 * rot[nkeys * zk + key]
                    t = pltpu.roll(t, kept, 1)
                    total = total + t
                    inside = inside + jnp.where(lane < kept, t, 0.0)
                wrapped = total - inside
                turned = swap(wrapped)
                main[s, p, ct] = main[s, p, ct] + (inside + jnp.where(low, turned, 0.0))
                if e == 0:
                    rim = rim + jnp.where(low, 0.0, turned)
                else:
                    rim = rim + jnp.where(low, wrapped, 0.0)
            rim_out[s, p, h] = rim
        if h is None:
            loop(cts // 2, pair)
        else:
            pair(h)

    def both(body):
        loop(2, body)

    def rims(s):
        both(lambda p: r_copy(s, p).start())

    def add_rim(s, p, h=None):
        r_copy(s, p, h).wait_recv()

        def pair(h):
            rim = rim_in[s, p, h]
            main[s, p, 2 * h] = main[s, p, 2 * h] + jnp.where(low, 0.0, rim)
            main[s, p, 2 * h + 1] = main[s, p, 2 * h + 1] + jnp.where(low, 0.0, swap(rim))
        if h is None:
            loop(cts // 2, pair)
        else:
            pair(h)

    def add_part(s, p, h=None):
        whole = view(part_in, s, p, h)
        e = 0 if h is None else h
        remote(whole, whole, o_send.at[0, p, e], o_recv.at[s, p, e], z, lb).wait_recv()
        at = (s, p) if h is None else (s, p, pl.ds(2 * h, 2))
        main[at] = main[at] + part_in[at]

    copy_d = pltpu.make_async_copy(digits, stage_d, local.at[0])
    copy_k = pltpu.make_async_copy(keys, stage_k, local.at[1])
    copy_d.start()
    copy_k.start()
    barrier = pltpu.get_barrier_semaphore()
    for zt, lt in ((zmod(z + 1), lb), (zmod(z + groups - 1), lb), (z, before), (z, after)):
        pl.semaphore_signal(barrier, inc=1, device_id=(zt, lt), device_id_type=MESH)

    row = lax.broadcasted_iota(jnp.int32, (rows, 128), 0)
    flag[...] = jnp.zeros_like(flag)
    flag[:cts, :requests.shape[1]] = requests[...].astype(f32)
    wanted = jnp.zeros((rows, 128), f32)
    for ct in range(cts):
        wanted = wanted + pltpu.roll(jnp.broadcast_to(flag[ct:ct + 1, :], (rows, 128)), 32 * ct, 1)
    wanted = jnp.concatenate([wanted] + [jnp.zeros((rows, 128), f32)] * (WIDE // 128 - 1), axis=1)
    for r in range(DEPTHS):
        dbuf[place(r, r), pages] = wanted
        m = jnp.ones((rows, 128), f32)
        for limb in range(LIMBS):
            value = mods[LIMBS * quarter(r) + limb].astype(f32)
            m = jnp.where((row == limb) | (row == limb + LIMBS), value, m)
        consts[r] = m
        consts[DEPTHS + r] = 1.0 / m

    def folded(x, r):
        first = lax.rem(quarter(r), 2) == 0
        a, b = x[:, :WIDE], x[:, WIDE:]
        return jnp.where(low, jnp.where(first, a, swap(a)), jnp.where(first, swap(b), b))

    def tile(r):
        return pl.ds(pl.multiple_of(rows * (quarter(r) // 2), rows), rows)

    copy_d.wait()
    pl.semaphore_wait(barrier, 4)
    for r in range(DEPTHS):
        def fold_d(ct):
            for j in range(dnum):
                dbuf[place(r, r), dnum * ct + j] = folded(stage_d[ct, j, tile(r), :], r)
        loop(cts, fold_d)
        d_copy(r, r).start()
    copy_k.wait()

    def fold_keys(r, p):
        def fold_k(key):
            for j in range(dnum):
                kbuf[place(r, r), p, key, j] = folded(stage_k[key, j, p, tile(r), :], r)
        loop(nkeys, fold_k)
    fold_keys(0, 0)
    k_copy(0, 0, 0).start()
    for r, p in ((1, 0), (2, 0), (3, 0), (0, 1), (1, 1), (2, 1), (3, 1)):
        fold_keys(r, p)

    def clear(i):
        s, p = i // 2, lax.rem(i, 2)
        main[s, p] = jnp.zeros(main.shape[2:], f32)
        rim_out[s, p] = jnp.zeros(rim_out.shape[2:], f32)
    loop(2 * SLOTS, clear)

    def own(i):
        r, p = i // 2, lax.rem(i, 2)
        unit(r * (r + 3) // 2, r, r, p)
    loop(2 * DEPTHS, own)
    rims(place(0, 0))

    def from_next(i, r0):
        r, p = r0 + i // 2, lax.rem(i, 2)
        unit(r * (r + 1) // 2 + r - 1, r, r, p)

    def block(s):
        both(lambda p: unit(s, LAST, LAST, p))
        rims(s)

    d_arrive(place(1, 0))
    d_copy(1, 0).start()
    k_copy(1, 1, 0).start()
    d_arrive(place(2, 1))
    d_copy(2, 1).start()
    loop(4, lambda i: from_next(i, 1))
    rims(place(1, 0))
    rims(place(2, 1))
    d_arrive(place(3, 2))
    d_copy(3, 2).start()
    block(place(3, 2))
    k_arrive(1, 0, 0)
    k_copy(1, 0, 0).start()
    d_arrive(place(2, 0))
    d_copy(2, 0).start()
    k_copy(2, 2, 0).start()
    d_arrive(CROSS + 3)
    both(lambda p: unit(CROSS + 3, LAST, LAST, p))
    both(lambda p: unit(place(2, 0), 2, 2, p))
    rims(place(2, 0))
    k_arrive(2, 1, 0)
    k_copy(2, 1, 0).start()
    d_arrive(place(3, 1))
    d_copy(3, 1).start()
    block(place(3, 1))
    d_arrive(CROSS + 2)
    both(lambda p: unit(CROSS + 2, LAST, LAST, p))
    d_arrive(place(3, 0))
    d_copy(3, 0).start()
    block(place(3, 0))
    k_arrive(2, 0, 0)
    k_copy(2, 0, 0).start()
    for r in (0, 1, 2):
        k_copy(r, r, 1).start()
    unit(place(1, 1), 1, 0, 0)
    r_copy(place(1, 1), 0).start()
    loop(2, lambda k: unit(place(2, 2), 2, k, 0))
    r_copy(place(2, 2), 0).start()
    for k in (2, 1):
        k_arrive(3, k, 0)
        unit(place(3, 3), LAST, k, 0)
        loop(2, lambda c: unit(CROSS + 2 + c, LAST, k, 0))

    def cross_block(c):
        loop(3, lambda i: unit(CROSS + c, LAST, LAST - i, 0))
        unit(CROSS + c, LAST, LAST, 1)
    for c in (1, 0):
        d_arrive(CROSS + c)
        cross_block(c)
    k_arrive(3, 0, 0)
    unit(place(3, 3), LAST, 0, 0)
    r_copy(place(3, 3), 0).start()

    def last_keys(c):
        unit(CROSS + c, LAST, 0, 0)
        r_copy(CROSS + c, 0).start()

    def leave(c):
        add_rim(CROSS + c, 0)
        o_cross(c, 0).start()

    def middle_keys(k):
        unit(place(3, 3), 3, k, 1)
        loop(DEPTHS, lambda c: unit(CROSS + c, LAST, k, 1))

    def pass_on(r, c, p):
        if p == 0:
            add_rim(place(r, c), p)
            add_part(place(r, c), p)
            o_copy(r, c, p).start()
        else:
            def half(h):
                add_part(place(r, c), p, h)
                o_copy(r, c, p, h).start()
            loop(2, half)

    loop(DEPTHS, last_keys)
    k_arrive(1, 0, 1)
    k_copy(1, 0, 1).start()
    unit(place(1, 1), 1, 0, 1)
    r_copy(place(1, 1), 1).start()
    k_arrive(2, 1, 1)
    k_copy(2, 1, 1).start()
    loop(DEPTHS, leave)
    unit(place(2, 2), 2, 1, 1)
    k_arrive(2, 0, 1)
    k_copy(2, 0, 1).start()
    unit(place(2, 2), 2, 0, 1)
    r_copy(place(2, 2), 1).start()
    k_arrive(3, 2, 1)
    middle_keys(2)
    for c in range(LAST):
        pass_on(3, c, 0)
    k_arrive(3, 1, 1)
    middle_keys(1)

    for r in range(1, DEPTHS):
        for c in range(r):
            add_rim(place(r, c), 1)
    k_arrive(3, 0, 1)

    def last_half(i):
        c, h = i // 2, lax.rem(i, 2)
        unit(CROSS + c, LAST, 0, 1, h)
        r_copy(CROSS + c, 1, h).start()
    loop(2 * DEPTHS, last_half)
    unit(place(3, 3), 3, 0, 1)
    r_copy(place(3, 3), 1).start()

    def leave_half(i):
        c, h = i // 2, lax.rem(i, 2)
        add_rim(CROSS + c, 1, h)
        o_cross(c, 1, h).start()

    def finish(r, p):
        s = place(r, r)
        add_rim(s, p)
        if p == 0:
            add_part(s, p)
        else:
            loop(2, lambda h: add_part(s, p, h))
        first = lax.rem(quarter(r), 2) == 0
        mine = low == first
        m, inv = tiled(consts[r]), tiled(consts[DEPTHS + r])

        def one(ct):
            v = main[s, p, ct]
            v = v - jnp.floor(v * inv) * m
            v = jnp.where(v < 0, v + m, v)
            v = jnp.where(v >= m, v - m, v) / m
            a = jnp.where(first, v, swap(v))
            b = jnp.where(first, swap(v), v)
            out[ct, p, tile(r), :WIDE] = jnp.where(mine, a, out[ct, p, tile(r), :WIDE])
            out[ct, p, tile(r), WIDE:] = jnp.where(mine, b, out[ct, p, tile(r), WIDE:])
        loop(cts, one)

    pass_on(2, 0, 0)
    loop(2, leave_half)
    pass_on(2, 1, 0)
    loop(2 * DEPTHS - 2, lambda i: leave_half(2 + i))
    pass_on(3, 0, 1)
    finish(3, 0)
    pass_on(1, 0, 0)
    pass_on(3, 1, 1)
    finish(2, 0)
    pass_on(2, 0, 1)
    pass_on(3, 2, 1)
    finish(1, 0)
    pass_on(2, 1, 1)
    pass_on(1, 0, 1)
    finish(0, 0)
    for r in (3, 2, 1, 0):
        finish(r, 1)

    def sent(copy):
        copy(0).wait_send()
        loop(2, lambda h: copy(1, h).wait_send())

    for r in range(DEPTHS):
        for c in range(r + 1):
            d_copy(r, c).wait_send()
            if r < LAST:
                both(lambda p: k_copy(r, c, p).wait_send())
            if c < r:
                sent(lambda *ph: o_copy(r, c, *ph))
    for c in range(DEPTHS):
        sent(lambda *ph: o_cross(c, *ph))
        sent(lambda *ph: r_copy(CROSS + c, *ph))
    loop(2 * CROSS, lambda i: r_copy(i // 2, lax.rem(i, 2)).wait_send())


def per_device(digits, keys, requests, rotations, moduli):
    groups, limbs = lax.axis_size("grp"), lax.axis_size("limb")
    cts, dnum, limb_count, columns = digits.shape
    nkeys = keys.shape[0]
    f32 = jnp.float32
    dma = pltpu.SemaphoreType.DMA
    smem = pl.BlockSpec(memory_space=pltpu.SMEM)
    vmem = pl.BlockSpec(memory_space=pltpu.VMEM)
    any_space = pl.BlockSpec(memory_space=pl.ANY)
    rows = 2 * LIMBS
    return pl.pallas_call(
        lambda *refs: kernel(groups, limbs, *refs),
        out_shape=jax.ShapeDtypeStruct((cts, 2, limb_count, columns), f32),
        in_specs=[smem, smem, any_space, any_space, vmem],
        out_specs=vmem,
        scratch_shapes=[
            pltpu.VMEM(digits.shape, f32),
            pltpu.VMEM(keys.shape, f32),
            pltpu.VMEM((2 * DEPTHS, rows, 128), f32),
            pltpu.VMEM((rows, 128), f32),
            pltpu.VMEM((SLOTS, cts * dnum + 1, rows, WIDE), f32),
            pltpu.VMEM((CROSS, 2, nkeys, dnum, rows, WIDE), f32),
            pltpu.VMEM((SLOTS, 2, cts, rows, WIDE), f32),
            pltpu.VMEM((CROSS, 2, cts, rows, WIDE), f32),
            pltpu.VMEM((SLOTS, 2, cts // 2, rows, WIDE), f32),
            pltpu.VMEM((SLOTS, 2, cts // 2, rows, WIDE), f32),
            dma((CROSS,)), dma((SLOTS,)),
            dma((CROSS, 2)), dma((CROSS, 2)),
            dma((SLOTS, 2, 2)), dma((CROSS, 2, 2)),
            dma((SLOTS, 2, 2)), dma((SLOTS, 2, 2)),
            dma((2,)),
        ],
        compiler_params=pltpu.CompilerParams(
            collective_id=0, has_side_effects=True, vmem_limit_bytes=60 * 1024 * 1024),
        name="keyswitch",
    )(rotations, moduli, digits, keys, requests)


def solution(mesh):
    in_specs = (
        P("grp", None, None, "limb"),
        P("grp", None, None, None, "limb"),
        P("grp", None),
        P(),
        P(),
    )
    out_specs = P("grp", None, None, "limb")
    return jax.shard_map(
        per_device, mesh=mesh, in_specs=in_specs, out_specs=out_specs, check_vma=False
    )
```
